32 devices in a mesh: tm: 8 (over y, x, core), batch: 4 (over z).
Axes of the slice: x: 2, y: 2, z: 4, core: 2. Of those that a mesh axis runs over, the one named last changes fastest.
Arguments:
- hidden_states: bfloat16 [4, 1024, 5120], P('batch', 'tm'), may hold values from -6 to 6
- gen_weight: bfloat16 [64, 5120], replicated, may hold values from -0.078125 to 0.078125
- noise_field: bfloat16 [4, 64, 1024], P('batch', None, 'tm'), may hold values from -6 to 6
- timesteps: int32 [4], P('batch'), may hold values from 200 to 999
- embed_real: bfloat16 [128, 5120], replicated, may hold values from -0.5 to 0.5
- time_real: bfloat16 [256, 3, 5120], P('tm'), may hold values from -0.375 to 0.375
- query_real: bfloat16 [5120, 1024], P(None, 'tm'), may hold values from -3 to 3
- key_real: bfloat16 [5120, 1024], P(None, 'tm'), may hold values from -3 to 3
- value_real: bfloat16 [5120, 1024], P(None, 'tm'), may hold values from -0.078125 to 0.078125
- out_real: bfloat16 [1024, 5120], P('tm'), may hold values from -0.1875 to 0.1875
- gain_real: float32 [2, 1024], P(None, 'tm'), may hold values from 0.25 to 3
- proj_real: bfloat16 [64, 5120], replicated, may hold values from -0.078125 to 0.078125
- embed_fake: bfloat16 [128, 5120], replicated, may hold values from -0.5 to 0.5
- time_fake: bfloat16 [256, 3, 5120], P('tm'), may hold values from -0.375 to 0.375
- query_fake: bfloat16 [5120, 1024], P(None, 'tm'), may hold values from -3 to 3
- key_fake: bfloat16 [5120, 1024], P(None, 'tm'), may hold values from -3 to 3
- value_fake: bfloat16 [5120, 1024], P(None, 'tm'), may hold values from -0.078125 to 0.078125
- out_fake: bfloat16 [1024, 5120], P('tm'), may hold values from -0.1875 to 0.1875
- gain_fake: float32 [2, 1024], P(None, 'tm'), may hold values from 0.25 to 3
- proj_fake: bfloat16 [64, 5120], replicated, may hold values from -0.078125 to 0.078125
Outputs:
- dmd_gradient: float32 [4, 64, 1024], P('batch', None, 'tm')
- weight_grad: float32 [64, 5120], replicated
The draws below stay inside these ranges and needn't reach their ends.
All inputs are finite; a program needn't handle non-finite values.
Results may differ from the reference program's by a relative error of at most 0.019.
Values may be sent and summed in bfloat16 or wider, within the bound.
A program may use at most 128 MiB of HBM per device.

```python
import math
import jax
import jax.numpy as jnp
from jax import lax

D = 5120
HD = 128
FREQ = 256
FTOK = 128
HEADS = 8
PATCH = 64
KIN = 128
TOKENS = 1024
SAMPLES = 4


def spiked_pair(key, salt_value):
    base_key = jax.random.fold_in(key, salt_value)
    key_one, key_two, key_three, key_four = jax.random.split(base_key, 4)
    proj_width = HEADS * HD
    query_draw = jax.random.normal(key_one, (D, proj_width), jnp.float32) / math.sqrt(D)
    key_draw = jax.random.normal(key_four, (D, proj_width), jnp.float32) / math.sqrt(D)
    return (jnp.clip(query_draw, -3.0, 3.0), jnp.clip(key_draw, -3.0, 3.0))


def draw_query_real(key, part):
    return spiked_pair(key, 11)[0].astype(jnp.bfloat16)


def draw_key_real(key, part):
    return spiked_pair(key, 11)[1].astype(jnp.bfloat16)


def draw_query_fake(key, part):
    return spiked_pair(key, 23)[0].astype(jnp.bfloat16)


def draw_key_fake(key, part):
    return spiked_pair(key, 23)[1].astype(jnp.bfloat16)


def touch_ends(drawn, key, smallest, largest):
    longest = drawn.shape.index(max(drawn.shape))
    spots = []
    for shift in (0, 1):
        where = [jax.random.randint(jax.random.fold_in(key, axis), (), 0, length) for axis, length in enumerate(drawn.shape)]
        where[longest] = (where[longest] + shift) % drawn.shape[longest]
        spots.append(tuple(where))
    return drawn.at[spots[0]].set(smallest).at[spots[1]].set(largest)


def level_of(key, extent, shards, low, top_value):
    def one(position, parts):
        steps = jax.random.uniform(jax.random.fold_in(jax.random.fold_in(key, 6), position), (parts,), jnp.float32, low / len(shards), top_value / len(shards))
        return jnp.repeat(jnp.exp(steps), extent[position] // parts).reshape((-1,) + (1,) * (len(extent) - position - 1))

    factor_of = one(*shards[0])
    for cut in shards[1:]:
        factor_of = factor_of * one(*cut)
    return factor_of


def scatter_about(rng, dims, deviation, most, cuts=(), kind=jnp.bfloat16):
    factor_of = level_of(rng, dims, cuts, -0.22, 0.18) if cuts else 1.0
    values = jax.random.normal(rng, dims, jnp.float32) * deviation * factor_of
    return jnp.minimum(jnp.maximum(values, -most), most).astype(kind)


def setup_inputs(seed: int = 0) -> dict:
    seeds = jax.random.split(jax.random.key(seed), 21)
    hidden_states = scatter_about(seeds[0], (SAMPLES, TOKENS, D), 1.0, 6.0, ((0, 4), (1, 8)))
    gen_weight = scatter_about(seeds[1], (PATCH, D), D ** -0.5, 0.078125)
    noise_field = scatter_about(seeds[2], (SAMPLES, PATCH, TOKENS), 1.0, 6.0, ((0, 4), (2, 8)))
    timesteps = touch_ends(jax.random.randint(seeds[3], (SAMPLES,), 200, 1000), jax.random.fold_in(seeds[3], 1), 200, 999).astype(jnp.int32)
    embed_real = scatter_about(seeds[4], (KIN, D), KIN ** -0.5, 0.5)
    time_real = scatter_about(seeds[5], (FREQ, 3, D), FREQ ** -0.5, 0.375, ((0, 8),))
    query_real = draw_query_real(jax.random.fold_in(seeds[20], 71), 0)
    key_real = draw_key_real(jax.random.fold_in(seeds[20], 71), 0)
    value_real = scatter_about(seeds[8], (D, HEADS * HD), D ** -0.5, 0.078125, ((1, 8),))
    out_real = scatter_about(seeds[9], (HEADS * HD, D), (HEADS * HD) ** -0.5, 0.1875, ((0, 8),))
    gain_real = jnp.clip(jnp.exp(math.log(3.0) - 2.4849066 * jax.random.uniform(seeds[10], (2, HEADS * HD), jnp.float32) ** level_of(seeds[10], (2, HEADS * HD), ((1, 8),), -0.2, 0.2)), 0.25, 3.0)
    proj_real = scatter_about(seeds[11], (PATCH, D), D ** -0.5, 0.078125)
    embed_fake = scatter_about(seeds[12], (KIN, D), KIN ** -0.5, 0.5)
    time_fake = scatter_about(seeds[13], (FREQ, 3, D), FREQ ** -0.5, 0.375, ((0, 8),))
    query_fake = draw_query_fake(jax.random.fold_in(seeds[20], 71), 0)
    key_fake = draw_key_fake(jax.random.fold_in(seeds[20], 71), 0)
    value_fake = scatter_about(seeds[16], (D, HEADS * HD), D ** -0.5, 0.078125, ((1, 8),))
    out_fake = scatter_about(seeds[17], (HEADS * HD, D), (HEADS * HD) ** -0.5, 0.1875, ((0, 8),))
    gain_fake = jnp.clip(jnp.exp(math.log(3.0) - 2.4849066 * jax.random.uniform(seeds[18], (2, HEADS * HD), jnp.float32) ** level_of(seeds[18], (2, HEADS * HD), ((1, 8),), -0.2, 0.2)), 0.25, 3.0)
    proj_fake = scatter_about(seeds[19], (PATCH, D), D ** -0.5, 0.078125)
    return dict(hidden_states=hidden_states, gen_weight=gen_weight, noise_field=noise_field, timesteps=timesteps, embed_real=embed_real, time_real=time_real, query_real=query_real, key_real=key_real, value_real=value_real, out_real=out_real, gain_real=gain_real, proj_real=proj_real, embed_fake=embed_fake, time_fake=time_fake, query_fake=query_fake, key_fake=key_fake, value_fake=value_fake, out_fake=out_fake, gain_fake=gain_fake, proj_fake=proj_fake)


norm_floor = 0.05
gap_floor = 0.25
highest = lax.Precision.HIGHEST

def sinusoid(time_step):
    half_freq = FREQ // 2
    frequency = jnp.exp(-math.log(10000.0) * jnp.arange(half_freq, dtype=jnp.float32) / half_freq)
    angles = time_step.astype(jnp.float32) * frequency
    return jnp.concatenate([jnp.cos(angles), jnp.sin(angles)]).astype(jnp.bfloat16)

def rms_round(vector, gain_row):
    return (vector * lax.rsqrt(lax.optimization_barrier(jnp.mean(vector * vector, axis=1, keepdims=True)) + norm_floor) * gain_row[None, :]).astype(jnp.bfloat16)

def velocity(noisy_patch, sinus_wave, embed_table, time_table, query_proj, key_proj, value_proj, out_proj, norm_gains, final_proj):
    earlier = jnp.concatenate([jnp.zeros((PATCH, FTOK), jnp.bfloat16), noisy_patch[:, :TOKENS - FTOK]], axis=1)
    stacked = jnp.concatenate([noisy_patch, earlier], axis=0)
    embedded = lax.dot_general(stacked, embed_table, (((0,), (0,)), ((), ())), preferred_element_type=jnp.float32)
    row_mean = lax.optimization_barrier(jnp.mean(embedded, axis=1, keepdims=True))
    centered = embedded - row_mean
    rscale = lax.rsqrt(lax.optimization_barrier(jnp.mean(centered * centered, axis=1, keepdims=True)) + norm_floor)
    modulation = jnp.einsum('f,fcd->cd', sinus_wave.astype(jnp.float32), time_table.astype(jnp.float32))
    normed = centered * rscale * (1.0 + modulation[1])[None, :] + modulation[0][None, :]
    queries = jnp.dot(normed, query_proj.astype(jnp.float32), precision=highest)
    keys_all = jnp.dot(normed, key_proj.astype(jnp.float32), precision=highest)
    values_all = jnp.dot(normed, value_proj.astype(jnp.float32), precision=highest).astype(jnp.bfloat16)
    query_norm = rms_round(queries, norm_gains[0])
    key_norm = rms_round(keys_all, norm_gains[1])
    frames = jnp.arange(TOKENS, dtype=jnp.int32) // FTOK
    allowed = frames[None, :] <= frames[:, None]

    def one_head(head_index):
        start_col = head_index * HD
        query_head = lax.dynamic_slice_in_dim(query_norm, start_col, HD, 1)
        key_head = lax.dynamic_slice_in_dim(key_norm, start_col, HD, 1)
        value_head = lax.dynamic_slice_in_dim(values_all, start_col, HD, 1)
        scores = jnp.dot(query_head, key_head.T, preferred_element_type=jnp.float32) / math.sqrt(HD)
        scores = jnp.where(allowed, scores, -1e+30)
        row_peak = lax.optimization_barrier(jnp.max(scores, axis=1, keepdims=True))
        exp_scores = jnp.exp(scores - row_peak)
        attn_probs = (exp_scores / lax.optimization_barrier(jnp.sum(exp_scores, axis=1, keepdims=True))).astype(jnp.bfloat16)
        return jnp.dot(attn_probs, value_head, preferred_element_type=jnp.float32).astype(jnp.bfloat16)
    per_head = lax.map(one_head, jnp.arange(HEADS, dtype=jnp.int32))
    attended = jnp.transpose(per_head, (1, 0, 2)).reshape(TOKENS, HEADS * HD)
    mixed = jnp.dot(attended, out_proj, preferred_element_type=jnp.float32)
    residual = embedded + mixed * modulation[2][None, :]
    return lax.dot_general(final_proj.astype(jnp.float32), residual, (((1,), (1,)), ((), ())), precision=highest)

def reference(hidden_states, gen_weight, noise_field, timesteps, embed_real, time_real, query_real, key_real, value_real, out_real, gain_real, proj_real, embed_fake, time_fake, query_fake, key_fake, value_fake, out_fake, gain_fake, proj_fake):
    grad_root = math.sqrt(SAMPLES * TOKENS)
    gradients = []
    grad_total = jnp.zeros((PATCH, D), jnp.float32)
    for sample in range(SAMPLES):
        time_step = timesteps[sample]
        level_raw = time_step.astype(jnp.float32) / 1000.0
        noise_level = 5.0 * level_raw / (1.0 + 4.0 * level_raw)
        generated = lax.dot_general(gen_weight, hidden_states[sample], (((1,), (1,)), ((), ())), preferred_element_type=jnp.float32).astype(jnp.bfloat16)
        noisy_patch = ((1.0 - noise_level) * generated.astype(jnp.float32) + noise_level * noise_field[sample].astype(jnp.float32)).astype(jnp.bfloat16)
        sinus_wave = sinusoid(time_step)
        vel_real = velocity(noisy_patch, sinus_wave, embed_real, time_real, query_real, key_real, value_real, out_real, gain_real, proj_real)
        vel_fake = velocity(noisy_patch, sinus_wave, embed_fake, time_fake, query_fake, key_fake, value_fake, out_fake, gain_fake, proj_fake)
        pred_real = noisy_patch.astype(jnp.float32) - noise_level * vel_real
        pred_fake = noisy_patch.astype(jnp.float32) - noise_level * vel_fake
        gap_mean = jnp.sum(jnp.abs(generated.astype(jnp.float32) - pred_real)) / (PATCH * TOKENS)
        normalizer = jnp.maximum(gap_mean, gap_floor)
        gap_diff = pred_fake - pred_real
        gradients.append(gap_diff / normalizer)
        difference = gap_diff.astype(jnp.bfloat16)
        partial_grad = jnp.dot(difference, hidden_states[sample], preferred_element_type=jnp.float32)
        grad_total = grad_total + partial_grad / normalizer / grad_root
    return (jnp.stack(gradients), grad_total)
```

```python
import functools
import math

import jax
import jax.numpy as jnp
import numpy as np
from jax import lax
from jax.experimental import pallas as pl
from jax.experimental.pallas import tpu as pltpu
from jax.sharding import PartitionSpec as P

HD = 128
FREQ = 256

norm_floor = 0.05
gap_floor = 0.25

MESH = pl.DeviceIdType.MESH
f32 = jnp.float32
bf16 = jnp.bfloat16


def hail(sizes):
    barrier = pltpu.get_barrier_semaphore()
    for axis, size in sizes.items():
        me = lax.axis_index(axis)
        for k in range(1, size):
            pl.semaphore_signal(
                barrier, inc=1, device_id={axis: lax.rem(me + k, size)}, device_id_type=MESH
            )


def meet(sizes):
    count = sum(size - 1 for size in sizes.values())
    pl.semaphore_wait(pltpu.get_barrier_semaphore(), count)


def partner(me, k, size):
    if size & (size - 1):
        return lax.rem(me + k, size)
    peer, bit = me, 1
    while bit < size:
        if k & bit:
            peer = peer + bit - 2 * bit * lax.rem(lax.div(me, bit), 2)
        bit *= 2
    return peer


def exchange(axis, size, source, slots, send, recv, hops=None):
    me = lax.axis_index(axis)
    copies = []
    for k in hops or range(1, size):
        peer = partner(me, k, size)
        copy = pltpu.make_async_remote_copy(
            src_ref=source(peer),
            dst_ref=slots.at[me],
            send_sem=send.at[k],
            recv_sem=recv.at[k],
            device_id={axis: peer},
            device_id_type=MESH,
        )
        copy.start()
        copies.append(copy)
    return copies


def landed(copies):
    for copy in copies:
        copy.wait_recv()


def gone(copies):
    for copy in copies:
        copy.wait_send()


def split(wide):
    high = wide.astype(bf16)
    return high, (wide - high.astype(f32)).astype(bf16)


def dot_nt(left, right):
    return lax.dot_general(left, right, (((1,), (1,)), ((), ())), preferred_element_type=f32)


def dot(left, right):
    return jnp.dot(left, right, preferred_element_type=f32)


LOADS = (
    "timesteps", "freqs", "time0", "time1", "hidden", "gen", "noise", "embed0", "proj0", "embed1",
    "proj1", "query0", "key0", "query1", "key1", "value0", "out0", "value1", "out1", "gain0", "gain1",
)


def main_kernel(n, nb, part, step, names, *refs):
    r = dict(zip(names, refs, strict=True))
    me = lax.axis_index("tm")
    mine = lax.axis_index("batch")
    core, chip = lax.rem(me, 2), lax.div(me, 2)
    chips = n // 2
    hidden, stack, modul = r["v_hidden"], r["stack"], r["modul"]
    noisy_ref = r["noisy"]
    patch_rows, frame = noisy_ref.shape
    tokens = n * frame
    kin = 2 * patch_rows
    width = hidden.shape[1]
    chunks = width // part
    steps, merge = width // step, step // part
    head = r["v_query0"].shape[1]
    freq_rows = r["v_time0"].shape[1]
    loads = {}
    for i, name in enumerate(LOADS):
        loads[name] = pltpu.make_async_copy(r[name], r["v_" + name], r["load_sem"].at[i])
        loads[name].start()
    hail({"tm": n, "batch": nb})

    def sem(name):
        return r["s_" + name], r["r_" + name]

    loads["timesteps"].wait()
    loads["freqs"].wait()
    half = r["v_freqs"].shape[1]
    time_step = jnp.full((16, half), r["v_timesteps"][0], jnp.int32).astype(f32)
    angles = time_step * r["v_freqs"][...]
    wave = jnp.concatenate([jnp.cos(angles), jnp.sin(angles)], axis=1).astype(bf16)
    raw = time_step[:8] * (1.0 / 1000.0)
    level = ((5.0 * raw) / (1.0 + 4.0 * raw))[:1, :1]
    picked = (2 * half, 3 * freq_rows)
    column = lax.rem(lax.broadcasted_iota(jnp.int32, picked, 1), freq_rows) + me * freq_rows
    chosen = (lax.broadcasted_iota(jnp.int32, picked, 0) == column).astype(f32).astype(bf16)
    own_wave = dot(wave, chosen)
    block_of = lax.broadcasted_iota(jnp.int32, own_wave.shape, 1) // freq_rows
    row_of = lax.broadcasted_iota(jnp.int32, own_wave.shape, 0)
    share = None
    for i in (0, 1):
        loads[f"time{i}"].wait()
        table = r[f"v_time{i}"]
        left = jnp.where(row_of == block_of + 3 * i, own_wave, 0.0).astype(bf16)
        if freq_rows % 16:
            for j in range(3):
                term = dot(left[:, j * freq_rows : (j + 1) * freq_rows], table[j])
                share = term if share is None else share + term
        else:
            term = dot(left, table[...].reshape(3 * freq_rows, width))
            share = term if share is None else share + term
    share_ref, parts = r["share"], r["parts"]
    for s in range(n):
        if s < chunks:
            share_ref[s] = share[:8, s * part : (s + 1) * part].astype(share_ref.dtype)
        else:
            share_ref[s] = jnp.zeros((8, part), share_ref.dtype)
    meet({"tm": n, "batch": nb})
    scatter = exchange("tm", n, lambda peer: share_ref.at[peer], parts, *sem("scatter"))
    parts[me] = share_ref[me]

    loads["hidden"].wait()
    loads["gen"].wait()
    loads["noise"].wait()
    made = dot_nt(hidden[...], r["v_gen"][...]).T.astype(bf16).astype(f32)
    noisy = ((1.0 - level) * made + level * r["v_noise"][...].astype(f32)).astype(bf16)
    noisy_ref[...] = noisy
    patches = r["patches"]
    spread = exchange("tm", n, lambda peer: noisy_ref, patches, *sem("spread"))
    patches[me] = noisy_ref[...]
    noisy = noisy.astype(f32)

    def columns(s):
        return pl.ds(pl.multiple_of(s * part, 128), part)

    def wide(s):
        return pl.ds(pl.multiple_of(s * step, 128), step)

    columns_held = r["columns"]
    pass_hidden = []

    def pass_on(hops):
        hops = [k for k in hops if k < n]
        if hops:
            pass_hidden.extend(
                exchange(
                    "tm", n, lambda peer: hidden.at[:, columns(lax.rem(peer, chunks))],
                    columns_held, *sem("pass"), hops,
                )
            )

    pass_on([1])

    gram = r["gram"]
    extra = kin + patch_rows

    def gram_of(i):
        embed, proj = r[f"v_embed{i}"], r[f"v_proj{i}"]
        loads[f"embed{i}"].wait()
        loads[f"proj{i}"].wait()
        gram[i] = jnp.zeros(gram.shape[1:], f32)
        ones = jnp.ones((16, step), bf16)

        def gram_step(s, carry):
            table = embed[:, wide(s)]
            gram[i] += dot_nt(jnp.concatenate([table, proj[:, wide(s)], ones], axis=0), table)
            return carry

        lax.fori_loop(0, steps, gram_step, 0)

    gram_of(0)
    landed(scatter)
    modul[me] = jnp.sum(parts[...].astype(f32), axis=0).astype(modul.dtype)
    collect = exchange("tm", n, lambda peer: modul.at[me], modul, *sem("collect"))
    pass_on([2, 4])
    columns_held[me] = hidden[:, columns(lax.rem(me, chunks))]
    gram_of(1)

    landed(spread)
    for s in range(n):
        at = slice(s * frame, (s + 1) * frame)
        now = patches[s]
        before = patches[s - 1] if s else jnp.zeros_like(now)
        both = jnp.concatenate([now, before], axis=0)
        stack[:kin, at] = both
        stack[kin:, at] = both
    block = 2 * frame
    blocks = [slice(s * block, (s + 1) * block) for s in range(tokens // block)]
    rscale = r["rscale"]
    means = []
    for i in (0, 1):
        mean_row = gram[i, extra : extra + 8] / width
        means.append(mean_row.T[:, :1])
        centered = gram[i, :kin] / width - means[i] * mean_row[:1]
        gram_pair = jnp.concatenate(split(centered), axis=1)
        for at in blocks:
            pair = stack[:, at]
            variance = jnp.sum(pair[:kin].astype(f32) * dot(gram_pair, pair), axis=0, keepdims=True)
            rscale[i : i + 1, at] = lax.rsqrt(jnp.maximum(variance, 0.0) + norm_floor)
    landed(collect)
    pass_on([3, 5])

    left_ref, fold, fold_v, gate_fold = r["left"], r["fold"], r["fold_v"], r["gate_fold"]
    qk, squares, square_parts = r["qk"], r["squares"], r["square_parts"]

    def rows_of(s, first, count):
        found = [modul[s * merge + g].astype(f32)[first : first + count] for g in range(merge)]
        return found[0] if merge == 1 else jnp.concatenate(found, axis=1)

    def fold_qk(i):
        embed, query, key = r[f"v_embed{i}"], r[f"v_query{i}"], r[f"v_key{i}"]
        loads[f"query{i}"].wait()
        loads[f"key{i}"].wait()
        fold[i] = jnp.zeros(fold.shape[1:], f32)
        line = lax.broadcasted_iota(jnp.int32, (16, step), 0)

        def fold_step(s, carry):
            at = wide(s)
            rows = rows_of(s, 3 * i, 2)
            shift, scale = rows[:1], rows[1:2]
            high = ((embed[:, at].astype(f32) - means[i]) * (1.0 + scale)).astype(bf16)
            shift_high, shift_low = split(shift)
            shifts = jnp.where(
                line == 0, shift_high.astype(f32), jnp.where(line == 1, shift_low.astype(f32), 0.0)
            ).astype(bf16)
            left = jnp.concatenate([high, shifts], axis=0)
            left_ref[i, :, at] = left
            fold[i] += dot(left, jnp.concatenate([query[at, :], key[at, :]], axis=1))
            return carry

        lax.fori_loop(0, steps, fold_step, 0)
        folded = jnp.concatenate(split(fold[i, :kin].T), axis=1)
        tail = fold[i, kin : kin + 8].T
        offset = tail[:, :1] + tail[:, 1:2]
        for at in blocks:
            full = dot(folded, stack[:, at]) * rscale[i : i + 1, at] + offset
            qk[i, :, at] = full
            for j in range(2):
                rows = full[j * head : (j + 1) * head]
                squares[i, j : j + 1, at] = jnp.sum(rows * rows, axis=0, keepdims=True)
        copies = exchange(
            "tm", n, lambda peer: squares.at[i], square_parts.at[i], *sem(f"sums{i}")
        )
        square_parts[i, me] = squares[i]
        return copies

    values = r["values"]

    def fold_values(i):
        value, out, proj = r[f"v_value{i}"], r[f"v_out{i}"], r[f"v_proj{i}"]
        loads[f"value{i}"].wait()
        loads[f"out{i}"].wait()
        fold_v[i] = jnp.zeros(fold_v.shape[1:], f32)
        gate_fold[i] = jnp.zeros(gate_fold.shape[1:], f32)

        def value_step(s, carry):
            at = wide(s)
            gate = rows_of(s, 3 * i + 2, 1)
            fold_v[i] += dot(left_ref[i, :, at], value[at, :])
            gate_fold[i] += dot_nt(out[:, at], (proj[:, at].astype(f32) * gate).astype(bf16))
            return carry

        lax.fori_loop(0, steps, value_step, 0)
        gate_high, gate_low = split(gate_fold[i].T)
        value_high, value_low = split(fold_v[i])
        both = dot_nt(jnp.concatenate([gate_high, gate_low], axis=0), value_high)
        joint = both[:patch_rows] + both[patch_rows:] + dot_nt(gate_high, value_low)
        offset = joint[:, kin : kin + 1] + joint[:, kin + 1 : kin + 2]
        pairs = jnp.concatenate(split(joint[:, :kin]), axis=1)
        for at in blocks:
            full = dot(pairs, stack[:, at]) * rscale[i : i + 1, at] + offset
            values[i, :patch_rows, at] = full.astype(bf16)
            values[i, patch_rows:, at] = jnp.ones((16, block), bf16)

    sums = [fold_qk(0), fold_qk(1)]
    pass_on([6, 7, *range(8, n)])
    fold_values(0)
    fold_values(1)

    groups = min(4, tokens // block)
    per_group = tokens // block // groups
    keys, terms, term_parts = r["keys"], r["terms"], r["term_parts"]

    def attend(i):
        landed(sums[i])
        inverse = lax.rsqrt(jnp.sum(square_parts[i], axis=0) / (head * n) + norm_floor)
        gain = r[f"v_gain{i}"]
        gains = gain[0:1, :] * gain[1:2, :]
        to_query = math.log2(math.e) / math.sqrt(HD)
        for at in blocks:
            gained = qk[i, head:, at] * inverse[1:2, at]
            keys[i, at, :] = (gained.T * gains).astype(bf16)
            r["queries"][i, :, at] = (qk[i, :head, at] * (inverse[:1, at] * to_query)).astype(bf16)
        for group in range(groups):
            length = (group + 1) * per_group * block
            low = length - per_group * block

            def block_step(b, carry):
                at = pl.ds(pl.multiple_of(b * block, block), block)
                scores = dot(keys[i, :length], r["queries"][i, :, at])
                shape = (length - low, block)
                key_frame = (lax.broadcasted_iota(jnp.int32, shape, 0) + low) // frame
                query_frame = (lax.broadcasted_iota(jnp.int32, shape, 1) + b * block) // frame
                edge = jnp.where(key_frame <= query_frame, scores[low:], -1e30)
                scores = jnp.concatenate([scores[:low], edge], axis=0) if low else edge
                peak = jnp.max(scores, axis=0, keepdims=True)
                powers = jnp.exp2(scores - peak).astype(bf16)
                summed = dot(values[i, :, :length], powers)
                term = (summed[:patch_rows] / summed[patch_rows : patch_rows + 1]).astype(bf16)
                for j in range(2):
                    terms[i, 2 * b + j] = term[:, j * frame : (j + 1) * frame]
                return carry

            if per_group == 1:
                block_step(group, 0)
            else:
                lax.fori_loop(group * per_group, (group + 1) * per_group, block_step, 0)
        copies = exchange(
            "tm", n, lambda peer: terms.at[i, peer], term_parts.at[i], *sem(f"give{i}")
        )
        term_parts[i, me] = terms[i, me]
        return copies

    for name in ("gain0", "gain1"):
        loads[name].wait()
    give = [attend(0), attend(1)]

    own = stack[:, pl.ds(pl.multiple_of(me * frame, frame), frame)]
    velocity = []
    for i in (0, 1):
        inner = jnp.concatenate(split(gram[i, kin:extra]), axis=1)
        velocity.append(dot(inner, own))
    for i in (0, 1):
        landed(give[i])
        velocity[i] = velocity[i] + jnp.sum(term_parts[i].astype(f32), axis=0)
    pred_real = noisy - level * velocity[0]
    pred_fake = noisy - level * velocity[1]
    difference = pred_fake - pred_real
    rounded, all_rounded, gap, gaps = r["rounded"], r["all_rounded"], r["gap"], r["gaps"]
    rounded[...] = difference.astype(bf16)
    difference_copies = exchange("tm", n, lambda peer: rounded, all_rounded, *sem("diff"))
    distance = jnp.abs(made - pred_real)
    distance = jnp.sum(jnp.sum(distance, axis=0, keepdims=True), axis=1, keepdims=True)
    gap[...] = jnp.broadcast_to(distance, gap.shape)
    gap_copies = exchange("tm", n, lambda peer: gap, gaps, *sem("gap"))
    gaps[me] = gap[...]
    all_rounded[me] = rounded[...]
    landed(pass_hidden)
    landed(difference_copies)
    total = None
    for s in range(0, n, 2):
        lefts = jnp.concatenate([all_rounded[s], all_rounded[s + 1]], axis=1)
        term = dot(lefts, columns_held[s : s + 2].reshape(2 * frame, part))
        total = term if total is None else total + term
    landed(gap_copies)
    normalizer = jnp.maximum(jnp.sum(gaps[...], axis=0) / (patch_rows * tokens), gap_floor)
    r["difference"][...] = difference / normalizer[:1, :1]
    total = total * (1.0 / (normalizer[:1, :1] * math.sqrt(nb * tokens)))
    mixed, quarters, merged, grad = r["mixed"], r["quarters"], r["merged"], r["grad"]
    mixed[...] = total.reshape(mixed.shape).astype(bf16)
    across = exchange("batch", nb, lambda peer: mixed.at[peer], quarters, *sem("across"))
    quarters[mine] = mixed[mine]
    landed(across)
    merged[mine] = jnp.sum(quarters[...].astype(f32), axis=0).astype(bf16)
    back = exchange("batch", nb, lambda peer: merged.at[mine], merged, *sem("back"))

    grad[core, chip, mine] = merged[mine]
    chain = []

    def to_chips(piece, k):
        copies = []
        for hop in range(1, chips):
            peer = partner(chip, hop, chips)
            copy = pltpu.make_async_remote_copy(
                src_ref=merged.at[piece],
                dst_ref=grad.at[core, chip, piece],
                send_sem=r["s_chain"].at[k * chips + hop],
                recv_sem=r["r_chain"].at[k * chips + hop],
                device_id={"tm": 2 * peer + core},
                device_id_type=MESH,
            )
            copy.start()
            copies.append(copy)
        return copies

    chain.append(to_chips(mine, 0))
    for k in range(1, nb):
        back[k - 1].wait_recv()
        piece = partner(mine, k, nb)
        grad[core, chip, piece] = merged[piece]
        chain.append(to_chips(piece, k))

    def to_partner(at, hop):
        copy = pltpu.make_async_remote_copy(
            src_ref=grad.at[core, at],
            dst_ref=grad.at[core, at],
            send_sem=r["s_share"].at[hop],
            recv_sem=r["r_share"].at[hop],
            device_id={"tm": me + 1 - 2 * core},
            device_id_type=MESH,
        )
        copy.start()
        return copy

    shares = [to_partner(chip, 0)]
    for hop in range(1, chips):
        for copies in chain:
            copies[hop - 1].wait_recv()
        shares.append(to_partner(partner(chip, hop, chips), hop))
    landed(shares)
    weight_ref = r["weight"]
    for s in range(chunks):
        piece = grad[s % 2, s // 2]
        weight_ref[:, s * part : (s + 1) * part] = piece.reshape(patch_rows, part)
    for copies in (
        scatter, spread, collect, pass_hidden, *sums, *give, difference_copies, gap_copies,
        across, back, *chain, shares,
    ):
        gone(copies)


def per_device(
    hidden_states,
    gen_weight,
    noise_field,
    timesteps,
    embed_real,
    time_real,
    query_real,
    key_real,
    value_real,
    out_real,
    gain_real,
    proj_real,
    embed_fake,
    time_fake,
    query_fake,
    key_fake,
    value_fake,
    out_fake,
    gain_fake,
    proj_fake,
):
    n = lax.axis_size("tm")
    nb = lax.axis_size("batch")
    frame = hidden_states.shape[1]
    tokens = frame * n
    patch_rows, width = gen_weight.shape
    part = -(-width // (n * 128)) * 128
    while width % part:
        part += 128
    chunks = width // part
    merge = max(m for m in range(1, chunks + 1) if chunks % m == 0 and m * part <= 1280 or m == 1)
    step = merge * part
    chips, quarter, head = n // 2, patch_rows // nb, query_real.shape[1]
    kin = 2 * patch_rows
    half = FREQ // 2
    freqs = np.exp(-math.log(10000.0) * np.arange(half, dtype=np.float64) / half).astype(np.float32)
    inputs = dict(
        timesteps=timesteps, freqs=jnp.asarray(np.broadcast_to(freqs, (16, half))),
        time0=time_real.transpose(1, 0, 2), time1=time_fake.transpose(1, 0, 2),
        hidden=hidden_states[0], gen=gen_weight, noise=noise_field[0],
        embed0=embed_real, proj0=proj_real, embed1=embed_fake, proj1=proj_fake,
        query0=query_real, key0=key_real, query1=query_fake, key1=key_fake,
        value0=value_real, out0=out_real, value1=value_fake, out1=out_fake,
        gain0=gain_real, gain1=gain_fake,
    )
    vm = pltpu.VMEM
    outputs = dict(
        difference=jax.ShapeDtypeStruct((patch_rows, frame), f32),
        weight=jax.ShapeDtypeStruct((patch_rows, width), bf16),
    )
    scratch = {}
    for name in LOADS:
        array = inputs[name]
        scratch["v_" + name] = (pltpu.SMEM if name == "timesteps" else vm)(array.shape, array.dtype)
    scratch.update(
        load_sem=pltpu.SemaphoreType.DMA((len(LOADS),)),
        patches=vm((n, patch_rows, frame), bf16),
        share=vm((n, 8, part), bf16),
        parts=vm((n, 8, part), bf16),
        modul=vm((n, 8, part), bf16),
        noisy=vm((patch_rows, frame), bf16),
        columns=vm((n, frame, part), bf16),
        gram=vm((2, kin + patch_rows + 16, kin), f32),
        stack=vm((2 * kin, tokens), bf16),
        rscale=vm((2, tokens), f32),
        left=vm((2, kin + 16, width), bf16),
        fold=vm((2, kin + 16, 2 * head), f32),
        fold_v=vm((2, kin + 16, head), f32),
        gate_fold=vm((2, head, patch_rows), f32),
        qk=vm((2, 2 * head, tokens), f32),
        squares=vm((2, 2, tokens), f32),
        square_parts=vm((2, n, 2, tokens), f32),
        values=vm((2, patch_rows + 16, tokens), bf16),
        keys=vm((2, tokens, head), bf16),
        queries=vm((2, head, tokens), bf16),
        terms=vm((2, n, patch_rows, frame), bf16),
        term_parts=vm((2, n, patch_rows, frame), bf16),
        gap=vm((8, 128), f32),
        gaps=vm((n, 8, 128), f32),
        rounded=vm((patch_rows, frame), bf16),
        all_rounded=vm((n, patch_rows, frame), bf16),
        mixed=vm((nb, quarter, part), bf16),
        quarters=vm((nb, quarter, part), bf16),
        merged=vm((nb, quarter, part), bf16),
        grad=vm((2, chips, nb, quarter, part), bf16),
    )
    for name, count in dict(
        scatter=n, spread=n, collect=n, sums0=n, sums1=n, give0=n, give1=n, diff=n, gap=n,
        across=nb, back=nb, chain=nb * chips, share=chips,
    ).items():
        scratch["s_" + name] = pltpu.SemaphoreType.DMA((count,))
        scratch["r_" + name] = pltpu.SemaphoreType.DMA((count,))
    scratch["s_pass"] = pltpu.SemaphoreType.DMA((n,))
    scratch["r_pass"] = pltpu.SemaphoreType.DMA((n,))
    names = (*inputs, *outputs, *scratch)
    difference, weight_grad = pl.pallas_call(
        functools.partial(main_kernel, n, nb, part, step, names),
        out_shape=list(outputs.values()),
        in_specs=[pl.BlockSpec(memory_space=pl.ANY)] * len(inputs),
        out_specs=[pl.BlockSpec(memory_space=pltpu.VMEM)] * 2,
        scratch_shapes=list(scratch.values()),
        compiler_params=pltpu.CompilerParams(
            collective_id=0, has_side_effects=True, vmem_limit_bytes=60 * 1024 * 1024
        ),
    )(*inputs.values())
    return (difference[None], weight_grad.astype(f32))


def solution(mesh):
    in_specs = (
        P("batch", "tm", None),
        P(),
        P("batch", None, "tm"),
        P("batch"),
        P(),
        P("tm", None, None),
        P(None, "tm"),
        P(None, "tm"),
        P(None, "tm"),
        P("tm", None),
        P(None, "tm"),
        P(),
        P(),
        P("tm", None, None),
        P(None, "tm"),
        P(None, "tm"),
        P(None, "tm"),
        P("tm", None),
        P(None, "tm"),
        P(),
    )
    out_specs = (P("batch", None, "tm"), P())
    return jax.shard_map(
        per_device, mesh=mesh, in_specs=in_specs, out_specs=out_specs, check_vma=False
    )
```

```python
import functools
import math

import jax
import jax.numpy as jnp
import numpy as np
from jax import lax
from jax.experimental import pallas as pl
from jax.experimental.pallas import tpu as pltpu
from jax.sharding import PartitionSpec as P

HD = 128
FREQ = 256

norm_floor = 0.05
gap_floor = 0.25

MESH = pl.DeviceIdType.MESH
f32 = jnp.float32
bf16 = jnp.bfloat16


def hail(sizes):
    barrier = pltpu.get_barrier_semaphore()
    for axis, size in sizes.items():
        me = lax.axis_index(axis)
        for k in range(1, size):
            pl.semaphore_signal(
                barrier, inc=1, device_id={axis: lax.rem(me + k, size)}, device_id_type=MESH
            )


def meet(sizes):
    count = sum(size - 1 for size in sizes.values())
    pl.semaphore_wait(pltpu.get_barrier_semaphore(), count)


def partner(me, k, size):
    if size & (size - 1):
        return lax.rem(me + k, size)
    peer, bit = me, 1
    while bit < size:
        if k & bit:
            peer = peer + bit - 2 * bit * lax.rem(lax.div(me, bit), 2)
        bit *= 2
    return peer


def exchange(axis, size, source, slots, send, recv, hops=None):
    me = lax.axis_index(axis)
    copies = []
    for k in hops or range(1, size):
        peer = partner(me, k, size)
        copy = pltpu.make_async_remote_copy(
            src_ref=source(peer),
            dst_ref=slots.at[me],
            send_sem=send.at[k],
            recv_sem=recv.at[k],
            device_id={axis: peer},
            device_id_type=MESH,
        )
        copy.start()
        copies.append(copy)
    return copies


def landed(copies):
    for copy in copies:
        copy.wait_recv()


def gone(copies):
    for copy in copies:
        copy.wait_send()


def split(wide):
    high = wide.astype(bf16)
    return high, (wide - high.astype(f32)).astype(bf16)


def repeat(steps, body):
    if steps == 1:
        body(0, 0)
    else:
        lax.fori_loop(0, steps, body, 0)


def dot_nt(left, right):
    return lax.dot_general(left, right, (((1,), (1,)), ((), ())), preferred_element_type=f32)


def dot(left, right):
    return jnp.dot(left, right, preferred_element_type=f32)


LOADS = (
    "freqs", "time0", "time1", "hidden", "gen", "noise", "embed0", "proj0", "embed1",
    "proj1", "query0", "key0", "query1", "key1", "value0", "out0", "value1", "out1", "gain0", "gain1",
)


def main_kernel(n, nb, part, step, names, *refs):
    r = dict(zip(names, refs, strict=True))
    me = lax.axis_index("tm")
    mine = lax.axis_index("batch")
    core, chip = lax.rem(me, 2), lax.div(me, 2)
    chips = n // 2
    hidden, stack, modul = r["v_hidden"], r["stack"], r["modul"]
    noisy_ref = r["noisy"]
    patch_rows, frame = noisy_ref.shape
    tokens = n * frame
    kin = 2 * patch_rows
    width = hidden.shape[1]
    chunks = width // part
    steps, merge = width // step, step // part
    head = r["v_query0"].shape[1]
    freq_rows = r["v_time0"].shape[1]
    loads = {}
    for i, name in enumerate(LOADS):
        loads[name] = pltpu.make_async_copy(r[name], r["v_" + name], r["load_sem"].at[i])
        loads[name].start()
    hail({"tm": n, "batch": nb})

    def sem(name):
        return r["s_" + name], r["r_" + name]

    loads["freqs"].wait()
    half = r["v_freqs"].shape[1]
    time_step = jnp.full((16, half), r["timesteps"][0], jnp.int32).astype(f32)
    angles = time_step * r["v_freqs"][...]
    wave = jnp.concatenate([jnp.cos(angles), jnp.sin(angles)], axis=1).astype(bf16)
    raw = time_step[:8] * (1.0 / 1000.0)
    level = ((5.0 * raw) / (1.0 + 4.0 * raw))[:1, :1]
    picked = (2 * half, 3 * freq_rows)
    column = lax.rem(lax.broadcasted_iota(jnp.int32, picked, 1), freq_rows) + me * freq_rows
    chosen = (lax.broadcasted_iota(jnp.int32, picked, 0) == column).astype(f32).astype(bf16)
    own_wave = dot(wave, chosen)
    block_of = lax.broadcasted_iota(jnp.int32, own_wave.shape, 1) // freq_rows
    row_of = lax.broadcasted_iota(jnp.int32, own_wave.shape, 0)
    share = None
    for i in (0, 1):
        loads[f"time{i}"].wait()
        table = r[f"v_time{i}"]
        left = jnp.where(row_of == block_of + 3 * i, own_wave, 0.0).astype(bf16)
        if freq_rows % 16:
            for j in range(3):
                term = dot(left[:, j * freq_rows : (j + 1) * freq_rows], table[j])
                share = term if share is None else share + term
        else:
            term = dot(left, table[...].reshape(3 * freq_rows, width))
            share = term if share is None else share + term
    share_ref, parts = r["share"], r["parts"]
    for s in range(n):
        if s < chunks:
            share_ref[s] = share[:8, s * part : (s + 1) * part].astype(share_ref.dtype)
        else:
            share_ref[s] = jnp.zeros((8, part), share_ref.dtype)
    meet({"tm": n, "batch": nb})
    scatter = exchange("tm", n, lambda peer: share_ref.at[peer], parts, *sem("scatter"))
    parts[me] = share_ref[me]

    loads["hidden"].wait()
    loads["gen"].wait()
    loads["noise"].wait()
    made = dot_nt(hidden[...], r["v_gen"][...]).T.astype(bf16).astype(f32)
    noisy = ((1.0 - level) * made + level * r["v_noise"][...].astype(f32)).astype(bf16)
    noisy_ref[...] = noisy
    patches = r["patches"]
    spread = exchange("tm", n, lambda peer: noisy_ref, patches, *sem("spread"))
    patches[me] = noisy_ref[...]
    noisy = noisy.astype(f32)

    def columns(s):
        return pl.ds(pl.multiple_of(s * part, 128), part)

    def wide(s):
        return slice(0, step) if steps == 1 else pl.ds(pl.multiple_of(s * step, 128), step)

    columns_held = r["columns"]
    pass_hidden = []

    def pass_on(hops):
        hops = [k for k in hops if k < n]
        if hops:
            pass_hidden.extend(
                exchange(
                    "tm", n, lambda peer: hidden.at[:, columns(lax.rem(peer, chunks))],
                    columns_held, *sem("pass"), hops,
                )
            )

    pass_on([1])

    gram = r["gram"]
    extra = kin + patch_rows

    def gram_of(i):
        embed, proj = r[f"v_embed{i}"], r[f"v_proj{i}"]
        loads[f"embed{i}"].wait()
        loads[f"proj{i}"].wait()
        gram[i] = jnp.zeros(gram.shape[1:], f32)
        ones = jnp.ones((16, step), bf16)

        def gram_step(s, carry):
            table = embed[:, wide(s)]
            gram[i] += dot_nt(jnp.concatenate([table, proj[:, wide(s)], ones], axis=0), table)
            return carry

        repeat(steps, gram_step)

    gram_of(0)
    landed(scatter)
    modul[me] = jnp.sum(parts[...].astype(f32), axis=0).astype(modul.dtype)
    collect = exchange("tm", n, lambda peer: modul.at[me], modul, *sem("collect"))
    pass_on([2, 4])
    columns_held[me] = hidden[:, columns(lax.rem(me, chunks))]
    gram_of(1)

    landed(spread)
    for s in range(n):
        at = slice(s * frame, (s + 1) * frame)
        now = patches[s]
        before = patches[s - 1] if s else jnp.zeros_like(now)
        both = jnp.concatenate([now, before], axis=0)
        stack[:kin, at] = both
        stack[kin:, at] = both
    block = 2 * frame
    blocks = [slice(s * block, (s + 1) * block) for s in range(tokens // block)]
    rscale = r["rscale"]
    means = []
    for i in (0, 1):
        mean_row = gram[i, extra : extra + 8] / width
        means.append(mean_row.T[:, :1])
        centered = gram[i, :kin] / width - means[i] * mean_row[:1]
        gram_pair = jnp.concatenate(split(centered), axis=1)
        for at in blocks:
            pair = stack[:, at]
            variance = jnp.sum(pair[:kin].astype(f32) * dot(gram_pair, pair), axis=0, keepdims=True)
            rscale[i : i + 1, at] = lax.rsqrt(jnp.maximum(variance, 0.0) + norm_floor)
    landed(collect)

    left_ref, fold, fold_v, gate_fold = r["left"], r["fold"], r["fold_v"], r["gate_fold"]
    qk, squares, square_parts = r["qk"], r["squares"], r["square_parts"]

    def rows_of(s, first, count):
        found = [modul[s * merge + g].astype(f32)[first : first + count] for g in range(merge)]
        return found[0] if merge == 1 else jnp.concatenate(found, axis=1)

    def fold_qk(i):
        embed, query, key = r[f"v_embed{i}"], r[f"v_query{i}"], r[f"v_key{i}"]
        loads[f"query{i}"].wait()
        loads[f"key{i}"].wait()
        fold[i] = jnp.zeros(fold.shape[1:], f32)
        line = lax.broadcasted_iota(jnp.int32, (16, step), 0)

        def fold_step(s, carry):
            at = wide(s)
            rows = rows_of(s, 3 * i, 2)
            shift, scale = rows[:1], rows[1:2]
            high = ((embed[:, at].astype(f32) - means[i]) * (1.0 + scale)).astype(bf16)
            shift_high, shift_low = split(shift)
            shifts = jnp.where(
                line == 0, shift_high.astype(f32), jnp.where(line == 1, shift_low.astype(f32), 0.0)
            ).astype(bf16)
            left_ref[i, :kin, at] = high
            left_ref[i, kin:, at] = shifts
            fold[i] += dot(
                left_ref[i, :, at], jnp.concatenate([query[at, :], key[at, :]], axis=1)
            )
            return carry

        repeat(steps, fold_step)
        folded = jnp.concatenate(split(fold[i, :kin].T), axis=1)
        tail = fold[i, kin : kin + 8].T
        offset = tail[:, :1] + tail[:, 1:2]
        for at in blocks:
            full = dot(folded, stack[:, at]) * rscale[i : i + 1, at] + offset
            qk[i, :, at] = full
            found = [full[j * head : (j + 1) * head] for j in range(2)]
            found = [jnp.sum(rows * rows, axis=0, keepdims=True) for rows in found]
            squares[i, :, at] = jnp.concatenate(found, axis=0).astype(squares.dtype)
        copies = exchange(
            "tm", n, lambda peer: squares.at[i], square_parts.at[i], *sem(f"sums{i}")
        )
        square_parts[i, me] = squares[i]
        return copies

    values = r["values"]

    def fold_values(i):
        value, out, proj = r[f"v_value{i}"], r[f"v_out{i}"], r[f"v_proj{i}"]
        loads[f"value{i}"].wait()
        loads[f"out{i}"].wait()
        fold_v[i] = jnp.zeros(fold_v.shape[1:], f32)
        gate_fold[i] = jnp.zeros(gate_fold.shape[1:], f32)

        def value_step(s, carry):
            at = wide(s)
            gate = rows_of(s, 3 * i + 2, 1)
            fold_v[i] += dot(left_ref[i, :, at], value[at, :])
            gate_fold[i] += dot_nt(out[:, at], (proj[:, at].astype(f32) * gate).astype(bf16))
            return carry

        repeat(steps, value_step)
        gate_high, gate_low = split(gate_fold[i].T)
        value_high, value_low = split(fold_v[i])
        both = dot_nt(jnp.concatenate([gate_high, gate_low], axis=0), value_high)
        joint = both[:patch_rows] + both[patch_rows:] + dot_nt(gate_high, value_low)
        offset = joint[:, kin : kin + 1] + joint[:, kin + 1 : kin + 2]
        pairs = jnp.concatenate(split(joint[:, :kin]), axis=1)
        for at in blocks:
            full = dot(pairs, stack[:, at]) * rscale[i : i + 1, at] + offset
            values[i, :patch_rows, at] = full.astype(bf16)
            values[i, patch_rows:, at] = jnp.ones((16, block), bf16)

    sums = [fold_qk(0)]
    pass_on([3, 5])
    sums.append(fold_qk(1))
    pass_on([6, *range(8, n)])
    fold_values(0)
    fold_values(1)

    groups = min(4, tokens // block)
    per_group = tokens // block // groups
    keys, terms, term_parts = r["keys"], r["terms"], r["term_parts"]

    def attend(i):
        landed(sums[i])
        inverse = lax.rsqrt(jnp.sum(square_parts[i].astype(f32), axis=0) / (head * n) + norm_floor)
        gain = r[f"v_gain{i}"]
        gains = gain[0:1, :] * gain[1:2, :]
        to_query = math.log2(math.e) / math.sqrt(HD)
        for at in blocks:
            gained = qk[i, head:, at] * inverse[1:2, at]
            keys[i, at, :] = (gained.T * gains).astype(bf16)
            r["queries"][i, :, at] = (qk[i, :head, at] * (inverse[:1, at] * to_query)).astype(bf16)
        for group in range(groups):
            length = (group + 1) * per_group * block
            low = length - per_group * block

            def block_step(b, carry):
                at = pl.ds(pl.multiple_of(b * block, block), block)
                scores = dot(keys[i, :length], r["queries"][i, :, at])
                shape = (length - low, block)
                key_frame = (lax.broadcasted_iota(jnp.int32, shape, 0) + low) // frame
                query_frame = (lax.broadcasted_iota(jnp.int32, shape, 1) + b * block) // frame
                edge = jnp.where(key_frame <= query_frame, scores[low:], -1e30)
                scores = jnp.concatenate([scores[:low], edge], axis=0) if low else edge
                peak = jnp.max(scores, axis=0, keepdims=True)
                powers = jnp.exp2(scores - peak).astype(bf16)
                summed = dot(values[i, :, :length], powers)
                term = (summed[:patch_rows] / summed[patch_rows : patch_rows + 1]).astype(bf16)
                for j in range(2):
                    terms[i, 2 * b + j] = term[:, j * frame : (j + 1) * frame]
                return carry

            if per_group == 1:
                block_step(group, 0)
            else:
                lax.fori_loop(group * per_group, (group + 1) * per_group, block_step, 0)
        copies = exchange(
            "tm", n, lambda peer: terms.at[i, peer], term_parts.at[i], *sem(f"give{i}")
        )
        term_parts[i, me] = terms[i, me]
        return copies

    for name in ("gain0", "gain1"):
        loads[name].wait()
    give = [attend(0), attend(1)]
    pass_on([7])

    own = stack[:, pl.ds(pl.multiple_of(me * frame, frame), frame)]
    velocity = []
    for i in (0, 1):
        inner = jnp.concatenate(split(gram[i, kin:extra]), axis=1)
        velocity.append(dot(inner, own))
    for i in (0, 1):
        landed(give[i])
        velocity[i] = velocity[i] + jnp.sum(term_parts[i].astype(f32), axis=0)
    pred_real = noisy - level * velocity[0]
    pred_fake = noisy - level * velocity[1]
    difference = pred_fake - pred_real
    rounded, all_rounded, gap, gaps = r["rounded"], r["all_rounded"], r["gap"], r["gaps"]
    rounded[...] = difference.astype(bf16)
    difference_copies = exchange("tm", n, lambda peer: rounded, all_rounded, *sem("diff"))
    distance = jnp.abs(made - pred_real)
    distance = jnp.sum(jnp.sum(distance, axis=0, keepdims=True), axis=1, keepdims=True)
    gap[...] = jnp.broadcast_to(distance, gap.shape)
    gap_copies = exchange("tm", n, lambda peer: gap, gaps, *sem("gap"))
    gaps[me] = gap[...]
    all_rounded[me] = rounded[...]
    landed(pass_hidden)
    landed(difference_copies)
    total = None
    for s in range(0, n, 2):
        lefts = jnp.concatenate([all_rounded[s], all_rounded[s + 1]], axis=1)
        term = dot(lefts, columns_held[s : s + 2].reshape(2 * frame, part))
        total = term if total is None else total + term
    landed(gap_copies)
    normalizer = jnp.maximum(jnp.sum(gaps[...], axis=0) / (patch_rows * tokens), gap_floor)
    r["difference"][...] = difference / normalizer[:1, :1]
    total = total * (1.0 / (normalizer[:1, :1] * math.sqrt(nb * tokens)))
    mixed, quarters, merged, grad = r["mixed"], r["quarters"], r["merged"], r["grad"]
    mixed[...] = total.reshape(mixed.shape).astype(bf16)
    across = exchange("batch", nb, lambda peer: mixed.at[peer], quarters, *sem("across"))
    quarters[mine] = mixed[mine]
    landed(across)
    merged[mine] = jnp.sum(quarters[...].astype(f32), axis=0).astype(bf16)
    back = exchange("batch", nb, lambda peer: merged.at[mine], merged, *sem("back"))

    grad[core, chip, mine] = merged[mine]
    chain = []

    def to_chips(piece, k):
        copies = []
        for hop in range(1, chips):
            peer = partner(chip, hop, chips)
            copy = pltpu.make_async_remote_copy(
                src_ref=merged.at[piece],
                dst_ref=grad.at[core, chip, piece],
                send_sem=r["s_chain"].at[k * chips + hop],
                recv_sem=r["r_chain"].at[k * chips + hop],
                device_id={"tm": 2 * peer + core},
                device_id_type=MESH,
            )
            copy.start()
            copies.append(copy)
        return copies

    chain.append(to_chips(mine, 0))
    for k in range(1, nb):
        back[k - 1].wait_recv()
        piece = partner(mine, k, nb)
        grad[core, chip, piece] = merged[piece]
        chain.append(to_chips(piece, k))

    def to_partner(at, hop):
        copy = pltpu.make_async_remote_copy(
            src_ref=grad.at[core, at],
            dst_ref=grad.at[core, at],
            send_sem=r["s_share"].at[hop],
            recv_sem=r["r_share"].at[hop],
            device_id={"tm": me + 1 - 2 * core},
            device_id_type=MESH,
        )
        copy.start()
        return copy

    shares = [to_partner(chip, 0)]
    for hop in range(1, chips):
        for copies in chain:
            copies[hop - 1].wait_recv()
        shares.append(to_partner(partner(chip, hop, chips), hop))
    landed(shares)
    for copies in (
        scatter, spread, collect, pass_hidden, *sums, *give, difference_copies, gap_copies,
        across, back, *chain, shares,
    ):
        gone(copies)


def last_kernel(part, grad_ref, difference_ref, weight_out, difference_out, wide_ref, sems):
    patch_rows, width = wide_ref.shape
    copies = [pltpu.make_async_copy(difference_ref, difference_out, sems.at[0])]
    copies[0].start()
    for s in range(width // part):
        at = slice(s * part, (s + 1) * part)
        wide_ref[:, at] = grad_ref[s % 2, s // 2].reshape(patch_rows, part).astype(f32)
        copies.append(
            pltpu.make_async_copy(wide_ref.at[:, at], weight_out.at[:, at], sems.at[s + 1])
        )
        copies[-1].start()
    for copy in copies:
        copy.wait()


def per_device(
    hidden_states,
    gen_weight,
    noise_field,
    timesteps,
    embed_real,
    time_real,
    query_real,
    key_real,
    value_real,
    out_real,
    gain_real,
    proj_real,
    embed_fake,
    time_fake,
    query_fake,
    key_fake,
    value_fake,
    out_fake,
    gain_fake,
    proj_fake,
):
    n = lax.axis_size("tm")
    nb = lax.axis_size("batch")
    frame = hidden_states.shape[1]
    tokens = frame * n
    patch_rows, width = gen_weight.shape
    part = -(-width // (n * 128)) * 128
    while width % part:
        part += 128
    chunks = width // part
    merge = max(m for m in range(1, chunks + 1) if chunks % m == 0 and m * part <= 5120 or m == 1)
    step = merge * part
    chips, quarter, head = n // 2, patch_rows // nb, query_real.shape[1]
    kin = 2 * patch_rows
    half = FREQ // 2
    freqs = np.exp(-math.log(10000.0) * np.arange(half, dtype=np.float64) / half).astype(np.float32)
    inputs = dict(
        freqs=jnp.asarray(np.broadcast_to(freqs, (16, half))),
        time0=time_real.transpose(1, 0, 2), time1=time_fake.transpose(1, 0, 2),
        hidden=hidden_states[0], gen=gen_weight, noise=noise_field[0],
        embed0=embed_real, proj0=proj_real, embed1=embed_fake, proj1=proj_fake,
        query0=query_real, key0=key_real, query1=query_fake, key1=key_fake,
        value0=value_real, out0=out_real, value1=value_fake, out1=out_fake,
        gain0=gain_real, gain1=gain_fake,
    )
    vm = pltpu.VMEM
    outputs = dict(
        difference=vm((patch_rows, frame), f32),
        grad=vm((2, chips, nb, quarter, part), bf16),
    )
    scratch = {}
    for name in LOADS:
        array = inputs[name]
        scratch["v_" + name] = vm(array.shape, array.dtype)
    scratch.update(
        load_sem=pltpu.SemaphoreType.DMA((len(LOADS),)),
        patches=vm((n, patch_rows, frame), bf16),
        share=vm((n, 8, part), bf16),
        parts=vm((n, 8, part), bf16),
        modul=vm((n, 8, part), bf16),
        noisy=vm((patch_rows, frame), bf16),
        columns=vm((n, frame, part), bf16),
        gram=vm((2, kin + patch_rows + 16, kin), f32),
        stack=vm((2 * kin, tokens), bf16),
        rscale=vm((2, tokens), f32),
        left=vm((2, kin + 16, width), bf16),
        fold=vm((2, kin + 16, 2 * head), f32),
        fold_v=vm((2, kin + 16, head), f32),
        gate_fold=vm((2, head, patch_rows), f32),
        qk=vm((2, 2 * head, tokens), f32),
        squares=vm((2, 2, tokens), bf16),
        square_parts=vm((2, n, 2, tokens), bf16),
        values=vm((2, patch_rows + 16, tokens), bf16),
        keys=vm((2, tokens, head), bf16),
        queries=vm((2, head, tokens), bf16),
        terms=vm((2, n, patch_rows, frame), bf16),
        term_parts=vm((2, n, patch_rows, frame), bf16),
        gap=vm((8, 128), f32),
        gaps=vm((n, 8, 128), f32),
        rounded=vm((patch_rows, frame), bf16),
        all_rounded=vm((n, patch_rows, frame), bf16),
        mixed=vm((nb, quarter, part), bf16),
        quarters=vm((nb, quarter, part), bf16),
        merged=vm((nb, quarter, part), bf16),
    )
    for name, count in dict(
        scatter=n, spread=n, collect=n, sums0=n, sums1=n, give0=n, give1=n, diff=n, gap=n,
        across=nb, back=nb, chain=nb * chips, share=chips,
    ).items():
        scratch["s_" + name] = pltpu.SemaphoreType.DMA((count,))
        scratch["r_" + name] = pltpu.SemaphoreType.DMA((count,))
    scratch["s_pass"] = pltpu.SemaphoreType.DMA((n,))
    scratch["r_pass"] = pltpu.SemaphoreType.DMA((n,))
    names = ("timesteps", *LOADS, *outputs, *scratch)
    difference, grad = pl.pallas_call(
        functools.partial(main_kernel, n, nb, part, step, names),
        out_shape=list(outputs.values()),
        in_specs=[pl.BlockSpec(memory_space=pltpu.SMEM)]
        + [pl.BlockSpec(memory_space=pltpu.HBM)] * len(LOADS),
        out_specs=[pl.BlockSpec(memory_space=pltpu.VMEM)] * 2,
        scratch_shapes=list(scratch.values()),
        compiler_params=pltpu.CompilerParams(
            collective_id=0, has_side_effects=True, vmem_limit_bytes=60 * 1024 * 1024
        ),
    )(timesteps, *(pltpu.with_memory_space_constraint(inputs[x], pltpu.HBM) for x in LOADS))
    weight_grad, difference = pl.pallas_call(
        functools.partial(last_kernel, part),
        out_shape=[
            jax.ShapeDtypeStruct((patch_rows, width), f32),
            jax.ShapeDtypeStruct((patch_rows, frame), f32),
        ],
        in_specs=[pl.BlockSpec(memory_space=pltpu.VMEM)] * 2,
        out_specs=[pl.BlockSpec(memory_space=pl.ANY)] * 2,
        scratch_shapes=[vm((patch_rows, width), f32), pltpu.SemaphoreType.DMA((chunks + 1,))],
        compiler_params=pltpu.CompilerParams(vmem_limit_bytes=8 * 1024 * 1024),
    )(*(pltpu.with_memory_space_constraint(x, pltpu.VMEM) for x in (grad, difference)))
    return (difference[None], weight_grad)


def solution(mesh):
    in_specs = (
        P("batch", "tm", None),
        P(),
        P("batch", None, "tm"),
        P("batch"),
        P(),
        P("tm", None, None),
        P(None, "tm"),
        P(None, "tm"),
        P(None, "tm"),
        P("tm", None),
        P(None, "tm"),
        P(),
        P(),
        P("tm", None, None),
        P(None, "tm"),
        P(None, "tm"),
        P(None, "tm"),
        P("tm", None),
        P(None, "tm"),
        P(),
    )
    out_specs = (P("batch", None, "tm"), P())
    return jax.shard_map(
        per_device, mesh=mesh, in_specs=in_specs, out_specs=out_specs, check_vma=False
    )
```

```python
import functools
import math

import jax
import jax.numpy as jnp
from jax import lax
from jax.experimental import pallas as pl
from jax.experimental.pallas import tpu as pltpu
from jax.sharding import PartitionSpec as P

HD = 128
FREQ = 256

norm_floor = 0.05
gap_floor = 0.25

MESH = pl.DeviceIdType.MESH
f32 = jnp.float32
bf16 = jnp.bfloat16


def hail(sizes):
    barrier = pltpu.get_barrier_semaphore()
    for axis, size in sizes.items():
        me = lax.axis_index(axis)
        for k in range(1, size):
            pl.semaphore_signal(
                barrier, inc=1, device_id={axis: lax.rem(me + k, size)}, device_id_type=MESH
            )


def meet(sizes):
    count = sum(size - 1 for size in sizes.values())
    pl.semaphore_wait(pltpu.get_barrier_semaphore(), count)


def partner(me, k, size):
    if size & (size - 1):
        return lax.rem(me + k, size)
    peer, bit = me, 1
    while bit < size:
        if k & bit:
            peer = peer + bit - 2 * bit * lax.rem(lax.div(me, bit), 2)
        bit *= 2
    return peer


class Exchange:
    def __init__(self, axis, size, source, slots, sems):
        self.axis, self.size, self.source, self.slots, self.sems = axis, size, source, slots, sems

    def start(self, hops=None):
        me = lax.axis_index(self.axis)
        for k in hops or range(1, self.size):
            if k < self.size:
                peer = partner(me, k, self.size)
                self.copy(self.source(peer), self.slots.at[me], peer).start()
        return self

    def copy(self, source, target, peer):
        return pltpu.make_async_remote_copy(
            src_ref=source,
            dst_ref=target,
            send_sem=self.sems[0].at[0],
            recv_sem=self.sems[1].at[0],
            device_id={self.axis: peer},
            device_id_type=MESH,
        )

    def all(self):
        both = self.slots.at[pl.ds(0, self.size - 1)]
        return self.copy(both, both, lax.axis_index(self.axis))


def exchange(axis, size, source, slots, sems):
    return Exchange(axis, size, source, slots, sems).start()


def landed(copies):
    copies.all().wait_recv()


def gone(copies):
    copies.all().wait_send()


def split(wide):
    high = wide.astype(bf16)
    return high, (wide - high.astype(f32)).astype(bf16)


def repeat(steps, body):
    if steps == 1:
        body(0, 0)
    else:
        lax.fori_loop(0, steps, body, 0)


def dot_nt(left, right):
    return lax.dot_general(left, right, (((1,), (1,)), ((), ())), preferred_element_type=f32)


def dot(left, right):
    return jnp.dot(left, right, preferred_element_type=f32)


LOADS = (
    "time0", "time1", "hidden", "gen", "noise", "embed0", "proj0", "embed1",
    "proj1", "query0", "key0", "query1", "key1", "value0", "out0", "value1", "out1", "gain0", "gain1",
)


def main_kernel(n, nb, part, step, names, *refs):
    r = dict(zip(names, refs, strict=True))
    me = lax.axis_index("tm")
    mine = lax.axis_index("batch")
    core, chip = lax.rem(me, 2), lax.div(me, 2)
    chips = n // 2
    hidden, stack, modul = r["v_hidden"], r["stack"], r["modul"]
    noisy_ref = r["noisy"]
    patch_rows, frame = noisy_ref.shape
    tokens = n * frame
    kin = 2 * patch_rows
    width = hidden.shape[1]
    chunks = width // part
    steps, merge = width // step, step // part
    head = r["v_query0"].shape[1]
    freq_rows = r["v_time0"].shape[1]
    loads = {}
    for i, name in enumerate(LOADS):
        loads[name] = pltpu.make_async_copy(r[name], r["v_" + name], r["load_sem"].at[i])
        loads[name].start()
    hail({"tm": n, "batch": nb})

    def sem(name):
        return r["s_" + name], r["r_" + name]

    half = FREQ // 2
    time_step = jnp.full((16, half), r["timesteps"][0], jnp.int32).astype(f32)
    place = lax.broadcasted_iota(jnp.int32, (16, half), 1)
    angles = time_step
    bit = 1
    while bit < half:
        factor = math.exp(-math.log(10000.0) * bit / half)
        angles = angles * jnp.where(lax.rem(lax.div(place, bit), 2) == 1, factor, 1.0)
        bit *= 2
    wave = jnp.concatenate([jnp.cos(angles), jnp.sin(angles)], axis=1).astype(bf16)
    raw = time_step[:8] * (1.0 / 1000.0)
    level = ((5.0 * raw) / (1.0 + 4.0 * raw))[:1, :1]
    picked = (2 * half, 3 * freq_rows)
    column = lax.rem(lax.broadcasted_iota(jnp.int32, picked, 1), freq_rows) + me * freq_rows
    chosen = (lax.broadcasted_iota(jnp.int32, picked, 0) == column).astype(f32).astype(bf16)
    own_wave = dot(wave, chosen)
    block_of = lax.broadcasted_iota(jnp.int32, own_wave.shape, 1) // freq_rows
    row_of = lax.broadcasted_iota(jnp.int32, own_wave.shape, 0)
    share = None
    for i in (0, 1):
        loads[f"time{i}"].wait()
        table = r[f"v_time{i}"]
        left = jnp.where(row_of == block_of + 3 * i, own_wave, 0.0).astype(bf16)
        if freq_rows % 16:
            for j in range(3):
                term = dot(left[:, j * freq_rows : (j + 1) * freq_rows], table[j])
                share = term if share is None else share + term
        else:
            term = dot(left, table[...].reshape(3 * freq_rows, width))
            share = term if share is None else share + term
    share_ref, parts = r["share"], r["parts"]
    for s in range(n):
        if s < chunks:
            share_ref[s] = share[:8, s * part : (s + 1) * part].astype(share_ref.dtype)
        else:
            share_ref[s] = jnp.zeros((8, part), share_ref.dtype)
    meet({"tm": n, "batch": nb})
    scatter = exchange("tm", n, lambda peer: share_ref.at[peer], parts, sem("scatter"))
    parts[me] = share_ref[me]

    loads["hidden"].wait()
    loads["gen"].wait()
    loads["noise"].wait()
    made = dot_nt(hidden[...], r["v_gen"][...]).T.astype(bf16).astype(f32)
    noisy = ((1.0 - level) * made + level * r["v_noise"][...].astype(f32)).astype(bf16)
    noisy_ref[...] = noisy
    patches = r["patches"]
    spread = exchange("tm", n, lambda peer: noisy_ref, patches, sem("spread"))
    patches[me] = noisy_ref[...]
    noisy = noisy.astype(f32)

    def columns(s):
        return pl.ds(pl.multiple_of(s * part, 128), part)

    def wide(s):
        return slice(0, step) if steps == 1 else pl.ds(pl.multiple_of(s * step, 128), step)

    columns_held = r["columns"]
    pass_hidden = Exchange(
        "tm", n, lambda peer: hidden.at[:, columns(lax.rem(peer, chunks))], columns_held, sem("pass")
    )
    pass_on = pass_hidden.start
    pass_on([1])

    gram = r["gram"]
    extra = kin + patch_rows

    def gram_of(i):
        embed, proj = r[f"v_embed{i}"], r[f"v_proj{i}"]
        loads[f"embed{i}"].wait()
        loads[f"proj{i}"].wait()
        gram[i] = jnp.zeros(gram.shape[1:], f32)
        ones = jnp.ones((16, step), bf16)

        def gram_step(s, carry):
            table = embed[:, wide(s)]
            gram[i] += dot_nt(jnp.concatenate([table, proj[:, wide(s)], ones], axis=0), table)
            return carry

        repeat(steps, gram_step)

    gram_of(0)
    landed(scatter)
    modul[me] = jnp.sum(parts[...].astype(f32), axis=0).astype(modul.dtype)
    collect = exchange("tm", n, lambda peer: modul.at[me], modul, sem("collect"))
    pass_on([2, 4])
    columns_held[me] = hidden[:, columns(lax.rem(me, chunks))]
    gram_of(1)

    landed(spread)
    for s in range(n):
        at = slice(s * frame, (s + 1) * frame)
        now = patches[s]
        before = patches[s - 1] if s else jnp.zeros_like(now)
        both = jnp.concatenate([now, before], axis=0)
        stack[:kin, at] = both
        stack[kin:, at] = both
    block = 2 * frame
    blocks = [slice(s * block, (s + 1) * block) for s in range(tokens // block)]
    rscale = r["rscale"]
    means = []
    for i in (0, 1):
        mean_row = gram[i, extra : extra + 8] / width
        means.append(mean_row.T[:, :1])
        centered = gram[i, :kin] / width - means[i] * mean_row[:1]
        gram_pair = jnp.concatenate(split(centered), axis=1)
        for at in blocks:
            pair = stack[:, at]
            variance = jnp.sum(pair[:kin].astype(f32) * dot(gram_pair, pair), axis=0, keepdims=True)
            rscale[i : i + 1, at] = lax.rsqrt(jnp.maximum(variance, 0.0) + norm_floor)
    landed(collect)

    left_ref, fold, fold_v, gate_fold = r["left"], r["fold"], r["fold_v"], r["gate_fold"]
    qk, squares, square_parts = r["qk"], r["squares"], r["square_parts"]

    def rows_of(s, first, count):
        found = [modul[s * merge + g].astype(f32)[first : first + count] for g in range(merge)]
        return found[0] if merge == 1 else jnp.concatenate(found, axis=1)

    def fold_qk(i):
        embed, query, key = r[f"v_embed{i}"], r[f"v_query{i}"], r[f"v_key{i}"]
        loads[f"query{i}"].wait()
        loads[f"key{i}"].wait()
        fold[i] = jnp.zeros(fold.shape[1:], f32)
        line = lax.broadcasted_iota(jnp.int32, (16, step), 0)

        def fold_step(s, carry):
            at = wide(s)
            rows = rows_of(s, 3 * i, 2)
            shift, scale = rows[:1], rows[1:2]
            high = ((embed[:, at].astype(f32) - means[i]) * (1.0 + scale)).astype(bf16)
            shift_high, shift_low = split(shift)
            shifts = jnp.where(
                line == 0, shift_high.astype(f32), jnp.where(line == 1, shift_low.astype(f32), 0.0)
            ).astype(bf16)
            left_ref[i, :kin, at] = high
            left_ref[i, kin:, at] = shifts
            fold[i] += dot(
                left_ref[i, :, at], jnp.concatenate([query[at, :], key[at, :]], axis=1)
            )
            return carry

        repeat(steps, fold_step)
        folded = jnp.concatenate(split(fold[i, :kin].T), axis=1)
        tail = fold[i, kin : kin + 8].T
        offset = tail[:, :1] + tail[:, 1:2]
        for at in blocks:
            full = dot(folded, stack[:, at]) * rscale[i : i + 1, at] + offset
            qk[i, :, at] = full
            found = [full[j * head : (j + 1) * head] for j in range(2)]
            found = [jnp.sum(rows * rows, axis=0, keepdims=True) for rows in found]
            squares[i, :, at] = jnp.concatenate(found, axis=0).astype(squares.dtype)
        copies = exchange(
            "tm", n, lambda peer: squares.at[i], square_parts.at[i], sem(f"sums{i}")
        )
        square_parts[i, me] = squares[i]
        return copies

    values = r["values"]

    def fold_values(i):
        value, out, proj = r[f"v_value{i}"], r[f"v_out{i}"], r[f"v_proj{i}"]
        loads[f"value{i}"].wait()
        loads[f"out{i}"].wait()
        fold_v[i] = jnp.zeros(fold_v.shape[1:], f32)
        gate_fold[i] = jnp.zeros(gate_fold.shape[1:], f32)

        def value_step(s, carry):
            at = wide(s)
            gate = rows_of(s, 3 * i + 2, 1)
            fold_v[i] += dot(left_ref[i, :, at], value[at, :])
            gate_fold[i] += dot_nt(out[:, at], (proj[:, at].astype(f32) * gate).astype(bf16))
            return carry

        repeat(steps, value_step)
        gate_high, gate_low = split(gate_fold[i].T)
        value_high, value_low = split(fold_v[i])
        both = dot_nt(jnp.concatenate([gate_high, gate_low], axis=0), value_high)
        joint = both[:patch_rows] + both[patch_rows:] + dot_nt(gate_high, value_low)
        offset = joint[:, kin : kin + 1] + joint[:, kin + 1 : kin + 2]
        pairs = jnp.concatenate(split(joint[:, :kin]), axis=1)
        for at in blocks:
            full = dot(pairs, stack[:, at]) * rscale[i : i + 1, at] + offset
            values[i, :patch_rows, at] = full.astype(bf16)
            values[i, patch_rows:, at] = jnp.ones((16, block), bf16)

    sums = [fold_qk(0)]
    pass_on([3, 5])
    sums.append(fold_qk(1))
    pass_on([6, *range(8, n)])
    fold_values(0)
    fold_values(1)

    groups = min(4, tokens // block)
    per_group = tokens // block // groups
    keys, terms, term_parts = r["keys"], r["terms"], r["term_parts"]

    def attend(i):
        landed(sums[i])
        inverse = lax.rsqrt(jnp.sum(square_parts[i].astype(f32), axis=0) / (head * n) + norm_floor)
        gain = r[f"v_gain{i}"]
        gains = gain[0:1, :] * gain[1:2, :]
        to_query = math.log2(math.e) / math.sqrt(HD)
        for at in blocks:
            gained = qk[i, head:, at] * inverse[1:2, at]
            keys[i, at, :] = (gained.T * gains).astype(bf16)
            r["queries"][i, :, at] = (qk[i, :head, at] * (inverse[:1, at] * to_query)).astype(bf16)
        for group in range(groups):
            length = (group + 1) * per_group * block
            low = length - per_group * block

            def block_step(b, carry):
                at = pl.ds(pl.multiple_of(b * block, block), block)
                scores = dot(keys[i, :length], r["queries"][i, :, at])
                shape = (length - low, block)
                key_frame = (lax.broadcasted_iota(jnp.int32, shape, 0) + low) // frame
                query_frame = (lax.broadcasted_iota(jnp.int32, shape, 1) + b * block) // frame
                edge = jnp.where(key_frame <= query_frame, scores[low:], -1e30)
                scores = jnp.concatenate([scores[:low], edge], axis=0) if low else edge
                peak = jnp.max(scores, axis=0, keepdims=True)
                powers = jnp.exp2(scores - peak).astype(bf16)
                summed = dot(values[i, :, :length], powers)
                term = (summed[:patch_rows] / summed[patch_rows : patch_rows + 1]).astype(bf16)
                for j in range(2):
                    terms[i, 2 * b + j] = term[:, j * frame : (j + 1) * frame]
                return carry

            if per_group == 1:
                block_step(group, 0)
            else:
                lax.fori_loop(group * per_group, (group + 1) * per_group, block_step, 0)
        copies = exchange(
            "tm", n, lambda peer: terms.at[i, peer], term_parts.at[i], sem(f"give{i}")
        )
        term_parts[i, me] = terms[i, me]
        return copies

    for name in ("gain0", "gain1"):
        loads[name].wait()
    give = [attend(0), attend(1)]
    pass_on([7])

    own = stack[:, pl.ds(pl.multiple_of(me * frame, frame), frame)]
    velocity = []
    for i in (0, 1):
        inner = jnp.concatenate(split(gram[i, kin:extra]), axis=1)
        velocity.append(dot(inner, own))
    for i in (0, 1):
        landed(give[i])
        velocity[i] = velocity[i] + jnp.sum(term_parts[i].astype(f32), axis=0)
    pred_real = noisy - level * velocity[0]
    pred_fake = noisy - level * velocity[1]
    difference = pred_fake - pred_real
    rounded, all_rounded, gap, gaps = r["rounded"], r["all_rounded"], r["gap"], r["gaps"]
    rounded[...] = difference.astype(bf16)
    difference_copies = exchange("tm", n, lambda peer: rounded, all_rounded, sem("diff"))
    distance = jnp.abs(made - pred_real)
    distance = jnp.sum(jnp.sum(distance, axis=0, keepdims=True), axis=1, keepdims=True)
    gap[...] = jnp.broadcast_to(distance, gap.shape)
    gap_copies = exchange("tm", n, lambda peer: gap, gaps, sem("gap"))
    gaps[me] = gap[...]
    all_rounded[me] = rounded[...]
    landed(pass_hidden)
    landed(difference_copies)
    total = None
    for s in range(0, n, 2):
        lefts = jnp.concatenate([all_rounded[s], all_rounded[s + 1]], axis=1)
        term = dot(lefts, columns_held[s : s + 2].reshape(2 * frame, part))
        total = term if total is None else total + term
    landed(gap_copies)
    normalizer = jnp.maximum(jnp.sum(gaps[...], axis=0) / (patch_rows * tokens), gap_floor)
    r["difference"][...] = difference / normalizer[:1, :1]
    total = total * (1.0 / (normalizer[:1, :1] * math.sqrt(nb * tokens)))
    mixed, quarters, merged, grad = r["mixed"], r["quarters"], r["merged"], r["grad"]
    mixed[...] = total.reshape(mixed.shape).astype(bf16)
    across = exchange("batch", nb, lambda peer: mixed.at[peer], quarters, sem("across"))
    quarters[mine] = mixed[mine]
    landed(across)
    merged[mine] = jnp.sum(quarters[...].astype(f32), axis=0).astype(bf16)
    grad[core, chip, mine] = merged[mine]

    def send(name, source, target, at, where):
        copy = pltpu.make_async_remote_copy(
            src_ref=source,
            dst_ref=target,
            send_sem=r["s_" + name].at[0],
            recv_sem=r["r_" + name].at[at],
            device_id=where,
            device_id_type=MESH,
        )
        return copy

    back = []
    for k in range(1, nb):
        back.append(
            send("back", merged.at[mine], merged.at[mine], k, {"batch": partner(mine, k, nb)})
        )
        back[-1].start()

    def to_chips(piece):
        for hop in range(1, chips):
            where = {"tm": 2 * partner(chip, hop, chips) + core}
            send("chain", merged.at[piece], grad.at[core, chip, piece], hop, where).start()

    to_chips(mine)
    for k in range(1, nb):
        back[k - 1].wait_recv()
        piece = partner(mine, k, nb)
        grad[core, chip, piece] = merged[piece]
        to_chips(piece)

    other = {"tm": me + 1 - 2 * core}

    def to_partner(at):
        send("share", grad.at[core, at], grad.at[core, at], 0, other).start()

    to_partner(chip)
    for hop in range(1, chips):
        at = partner(chip, hop, chips)
        send("chain", grad.at[core, at], grad.at[core, at], hop, other).wait_recv()
        to_partner(at)
    whole = send("share", grad.at[core], grad.at[1 - core], 0, other)
    whole.wait_recv()
    for copies in (
        scatter, spread, collect, pass_hidden, *sums, *give, difference_copies, gap_copies, across,
    ):
        gone(copies)
    rest = merged.at[pl.ds(0, nb - 1)]
    send("back", rest, rest, 0, other).wait_send()
    for hop in range(1, chips):
        send("chain", merged, merged, 0, other).wait_send()
    whole.wait_send()


def last_kernel(part, grad_ref, difference_ref, weight_out, difference_out, wide_ref, sems):
    patch_rows, width = wide_ref.shape
    copies = [pltpu.make_async_copy(difference_ref, difference_out, sems.at[0])]
    copies[0].start()
    for s in range(width // part):
        at = slice(s * part, (s + 1) * part)
        wide_ref[:, at] = grad_ref[s % 2, s // 2].reshape(patch_rows, part).astype(f32)
        copies.append(
            pltpu.make_async_copy(wide_ref.at[:, at], weight_out.at[:, at], sems.at[s + 1])
        )
        copies[-1].start()
    for copy in copies:
        copy.wait()


def per_device(
    hidden_states,
    gen_weight,
    noise_field,
    timesteps,
    embed_real,
    time_real,
    query_real,
    key_real,
    value_real,
    out_real,
    gain_real,
    proj_real,
    embed_fake,
    time_fake,
    query_fake,
    key_fake,
    value_fake,
    out_fake,
    gain_fake,
    proj_fake,
):
    n = lax.axis_size("tm")
    nb = lax.axis_size("batch")
    frame = hidden_states.shape[1]
    tokens = frame * n
    patch_rows, width = gen_weight.shape
    part = -(-width // (n * 128)) * 128
    while width % part:
        part += 128
    chunks = width // part
    merge = max(m for m in range(1, chunks + 1) if chunks % m == 0 and m * part <= 5120 or m == 1)
    step = merge * part
    chips, quarter, head = n // 2, patch_rows // nb, query_real.shape[1]
    kin = 2 * patch_rows
    inputs = dict(
        time0=time_real.transpose(1, 0, 2), time1=time_fake.transpose(1, 0, 2),
        hidden=hidden_states[0], gen=gen_weight, noise=noise_field[0],
        embed0=embed_real, proj0=proj_real, embed1=embed_fake, proj1=proj_fake,
        query0=query_real, key0=key_real, query1=query_fake, key1=key_fake,
        value0=value_real, out0=out_real, value1=value_fake, out1=out_fake,
        gain0=gain_real, gain1=gain_fake,
    )
    vm = pltpu.VMEM
    outputs = dict(
        difference=vm((patch_rows, frame), f32),
        grad=vm((2, chips, nb, quarter, part), bf16),
    )
    scratch = {}
    for name in LOADS:
        array = inputs[name]
        scratch["v_" + name] = vm(array.shape, array.dtype)
    scratch.update(
        load_sem=pltpu.SemaphoreType.DMA((len(LOADS),)),
        patches=vm((n, patch_rows, frame), bf16),
        share=vm((n, 8, part), bf16),
        parts=vm((n, 8, part), bf16),
        modul=vm((n, 8, part), bf16),
        noisy=vm((patch_rows, frame), bf16),
        columns=vm((n, frame, part), bf16),
        gram=vm((2, kin + patch_rows + 16, kin), f32),
        stack=vm((2 * kin, tokens), bf16),
        rscale=vm((2, tokens), f32),
        left=vm((2, kin + 16, width), bf16),
        fold=vm((2, kin + 16, 2 * head), f32),
        fold_v=vm((2, kin + 16, head), f32),
        gate_fold=vm((2, head, patch_rows), f32),
        qk=vm((2, 2 * head, tokens), f32),
        squares=vm((2, 2, tokens), bf16),
        square_parts=vm((2, n, 2, tokens), bf16),
        values=vm((2, patch_rows + 16, tokens), bf16),
        keys=vm((2, tokens, head), bf16),
        queries=vm((2, head, tokens), bf16),
        terms=vm((2, n, patch_rows, frame), bf16),
        term_parts=vm((2, n, patch_rows, frame), bf16),
        gap=vm((8, 128), f32),
        gaps=vm((n, 8, 128), f32),
        rounded=vm((patch_rows, frame), bf16),
        all_rounded=vm((n, patch_rows, frame), bf16),
        mixed=vm((nb, quarter, part), bf16),
        quarters=vm((nb, quarter, part), bf16),
        merged=vm((nb, quarter, part), bf16),
    )
    for name, count in dict(
        scatter=1, spread=1, collect=1, sums0=1, sums1=1, give0=1, give1=1, diff=1, gap=1,
        across=1, back=nb, chain=chips, share=1, **{"pass": 1},
    ).items():
        scratch["s_" + name] = pltpu.SemaphoreType.DMA((1,))
        scratch["r_" + name] = pltpu.SemaphoreType.DMA((count,))
    names = ("timesteps", *LOADS, *outputs, *scratch)
    difference, grad = pl.pallas_call(
        functools.partial(main_kernel, n, nb, part, step, names),
        out_shape=list(outputs.values()),
        in_specs=[pl.BlockSpec(memory_space=pltpu.SMEM)]
        + [pl.BlockSpec(memory_space=pltpu.HBM)] * len(LOADS),
        out_specs=[pl.BlockSpec(memory_space=pltpu.VMEM)] * 2,
        scratch_shapes=list(scratch.values()),
        compiler_params=pltpu.CompilerParams(
            collective_id=0, has_side_effects=True, vmem_limit_bytes=60 * 1024 * 1024
        ),
    )(timesteps, *(pltpu.with_memory_space_constraint(inputs[x], pltpu.HBM) for x in LOADS))
    weight_grad, difference = pl.pallas_call(
        functools.partial(last_kernel, part),
        out_shape=[
            jax.ShapeDtypeStruct((patch_rows, width), f32),
            jax.ShapeDtypeStruct((patch_rows, frame), f32),
        ],
        in_specs=[pl.BlockSpec(memory_space=pltpu.VMEM)] * 2,
        out_specs=[pl.BlockSpec(memory_space=pl.ANY)] * 2,
        scratch_shapes=[vm((patch_rows, width), f32), pltpu.SemaphoreType.DMA((chunks + 1,))],
        compiler_params=pltpu.CompilerParams(vmem_limit_bytes=8 * 1024 * 1024),
    )(*(pltpu.with_memory_space_constraint(x, pltpu.VMEM) for x in (grad, difference)))
    return (difference[None], weight_grad)


def solution(mesh):
    in_specs = (
        P("batch", "tm", None),
        P(),
        P("batch", None, "tm"),
        P("batch"),
        P(),
        P("tm", None, None),
        P(None, "tm"),
        P(None, "tm"),
        P(None, "tm"),
        P("tm", None),
        P(None, "tm"),
        P(),
        P(),
        P("tm", None, None),
        P(None, "tm"),
        P(None, "tm"),
        P(None, "tm"),
        P("tm", None),
        P(None, "tm"),
        P(),
    )
    out_specs = (P("batch", None, "tm"), P())
    return jax.shard_map(
        per_device, mesh=mesh, in_specs=in_specs, out_specs=out_specs, check_vma=False
    )
```

```python
import functools
import math

import jax
import jax.numpy as jnp
from jax import lax
from jax.experimental import pallas as pl
from jax.experimental.pallas import tpu as pltpu
from jax.sharding import PartitionSpec as P

HD = 128
FREQ = 256

norm_floor = 0.05
gap_floor = 0.25

MESH = pl.DeviceIdType.MESH
f32 = jnp.float32
bf16 = jnp.bfloat16


def hail(sizes):
    barrier = pltpu.get_barrier_semaphore()
    for axis, size in sizes.items():
        me = lax.axis_index(axis)
        for k in range(1, size):
            pl.semaphore_signal(
                barrier, inc=1, device_id={axis: lax.rem(me + k, size)}, device_id_type=MESH
            )


def meet(sizes):
    count = sum(size - 1 for size in sizes.values())
    pl.semaphore_wait(pltpu.get_barrier_semaphore(), count)


def partner(me, k, size):
    if size & (size - 1):
        return lax.rem(me + k, size)
    peer, bit = me, 1
    while bit < size:
        if k & bit:
            peer = peer + bit - 2 * bit * lax.rem(lax.div(me, bit), 2)
        bit *= 2
    return peer


class Exchange:
    def __init__(self, axis, size, source, slots, sems):
        self.axis, self.size, self.source, self.slots, self.sems = axis, size, source, slots, sems

    def start(self, hops=None):
        me = lax.axis_index(self.axis)
        for k in hops or range(1, self.size):
            if k < self.size:
                peer = partner(me, k, self.size)
                self.copy(self.source(peer), self.slots.at[me], peer).start()
        return self

    def copy(self, source, target, peer):
        return pltpu.make_async_remote_copy(
            src_ref=source,
            dst_ref=target,
            send_sem=self.sems[0].at[0],
            recv_sem=self.sems[1].at[0],
            device_id={self.axis: peer},
            device_id_type=MESH,
        )

    def all(self):
        both = self.slots.at[pl.ds(0, self.size - 1)]
        return self.copy(both, both, lax.axis_index(self.axis))


def exchange(axis, size, source, slots, sems):
    return Exchange(axis, size, source, slots, sems).start()


def landed(copies):
    copies.all().wait_recv()


def gone(copies):
    copies.all().wait_send()


def split(wide):
    high = wide.astype(bf16)
    return high, (wide - high.astype(f32)).astype(bf16)


def dot_nt(left, right):
    return lax.dot_general(left, right, (((1,), (1,)), ((), ())), preferred_element_type=f32)


def dot(left, right):
    return jnp.dot(left, right, preferred_element_type=f32)


LOADS = (
    "time0", "time1", "hidden", "gen", "noise", "embed0", "proj0", "embed1",
    "proj1", "query0", "key0", "query1", "key1", "value0", "out0", "value1", "out1", "gain0", "gain1",
)


def main_kernel(n, nb, part, names, *refs):
    r = dict(zip(names, refs, strict=True))
    me = lax.axis_index("tm")
    mine = lax.axis_index("batch")
    core, chip = lax.rem(me, 2), lax.div(me, 2)
    chips = n // 2
    hidden, stack = r["v_hidden"], r["stack"]
    noisy_ref = r["noisy"]
    patch_rows, frame = noisy_ref.shape
    tokens = n * frame
    kin = 2 * patch_rows
    width = hidden.shape[1]
    chunks = width // part
    head = r["v_query0"].shape[1]
    freq_rows = r["v_time0"].shape[1]
    loads = {}
    for i, name in enumerate(LOADS):
        loads[name] = pltpu.make_async_copy(r[name], r["v_" + name], r["load_sem"].at[i])
        loads[name].start()
    hail({"tm": n, "batch": nb})

    def sem(name):
        return r["s_" + name], r["r_" + name]

    half = FREQ // 2
    time_step = jnp.full((16, half), r["timesteps"][0], jnp.int32).astype(f32)
    place = lax.broadcasted_iota(jnp.int32, (16, half), 1)
    angles = time_step
    bit = 1
    while bit < half:
        factor = math.exp(-math.log(10000.0) * bit / half)
        angles = angles * jnp.where(lax.rem(lax.div(place, bit), 2) == 1, factor, 1.0)
        bit *= 2
    wave = jnp.concatenate([jnp.cos(angles), jnp.sin(angles)], axis=1).astype(bf16)
    raw = time_step[:8] * (1.0 / 1000.0)
    level = ((5.0 * raw) / (1.0 + 4.0 * raw))[:1, :1]
    picked = (2 * half, 3 * freq_rows)
    column = lax.rem(lax.broadcasted_iota(jnp.int32, picked, 1), freq_rows) + me * freq_rows
    chosen = (lax.broadcasted_iota(jnp.int32, picked, 0) == column).astype(f32).astype(bf16)
    own_wave = dot(wave, chosen)
    own_wave = jnp.concatenate([own_wave, own_wave], axis=0)
    block_of = lax.broadcasted_iota(jnp.int32, own_wave.shape, 1) // freq_rows
    row_of = lax.broadcasted_iota(jnp.int32, own_wave.shape, 0)
    share = None
    for i in (0, 1):
        loads[f"time{i}"].wait()
        table = r[f"v_time{i}"]
        early = (row_of // 8 == i) & (lax.rem(row_of, 2) == block_of)
        late = (row_of // 8 == 2) & (lax.rem(row_of, 2) == i) & (block_of == 2)
        left = jnp.where(early | late, own_wave, 0.0).astype(bf16)
        if freq_rows % 16:
            for j in range(3):
                term = dot(left[:, j * freq_rows : (j + 1) * freq_rows], table[j])
                share = term if share is None else share + term
        else:
            term = dot(left, table[...].reshape(3 * freq_rows, width))
            share = term if share is None else share + term
    pieces, piece_parts = r["pieces"], r["piece_parts"]
    some = width // 4
    line = lax.broadcasted_iota(jnp.int32, (8, some), 0) // 2
    for g in range(3):
        rows = share[8 * g : 8 * g + 8]
        picked = rows[:, :some]
        for q in range(1, 4):
            picked = jnp.where(line == q, rows[:, q * some : (q + 1) * some], picked)
        pieces[g] = picked.astype(bf16)
    meet({"tm": n, "batch": nb})

    def hand_on(g):
        copies = exchange("tm", n, lambda peer: pieces.at[g], piece_parts.at[g], sem(f"piece{g}"))
        piece_parts[g, me] = pieces[g]
        return copies

    piece_copies = [hand_on(0)]

    loads["hidden"].wait()
    loads["gen"].wait()
    loads["noise"].wait()
    made = dot_nt(hidden[...], r["v_gen"][...]).T.astype(bf16).astype(f32)
    noisy = ((1.0 - level) * made + level * r["v_noise"][...].astype(f32)).astype(bf16)
    noisy_ref[...] = noisy
    patches = r["patches"]
    spread = exchange("tm", n, lambda peer: noisy_ref, patches, sem("spread"))
    patches[me] = noisy_ref[...]
    piece_copies.extend([hand_on(1), hand_on(2)])
    noisy = noisy.astype(f32)

    def columns(s):
        return pl.ds(pl.multiple_of(s * part, 128), part)

    held = r["held"]
    other = {"tm": me + 1 - 2 * core}

    def send(name, source, target, at, where, slot=0):
        return pltpu.make_async_remote_copy(
            src_ref=source,
            dst_ref=target,
            send_sem=r["s_" + name].at[slot],
            recv_sem=r["r_" + name].at[at],
            device_id=where,
            device_id_type=MESH,
        )

    def part_of(q, side):
        return columns(lax.rem(2 * q + side, chunks))

    gram = r["gram"]
    extra = kin + patch_rows

    def gram_of(i):
        embed, proj = r[f"v_embed{i}"], r[f"v_proj{i}"]
        loads[f"embed{i}"].wait()
        loads[f"proj{i}"].wait()
        ones = jnp.ones((16, width), bf16)
        gram[i] = dot_nt(jnp.concatenate([embed[...], proj[...], ones], axis=0), embed[...])

    gram_of(0)
    for q in range(chips):
        send("held", hidden.at[:, part_of(q, 1 - core)], held.at[q], 0, other).start()
    gram_of(1)

    block = 2 * frame
    blocks = [slice(s * block, (s + 1) * block) for s in range(tokens // block)]
    rscale = r["rscale"]
    means, centered = [], []
    for i in (0, 1):
        mean_row = gram[i, extra : extra + 8] / width
        means.append(mean_row.T[:, :1])
        centered.append(gram[i, :kin] / width - means[i] * mean_row[:1])

    left_ref, fold, fold_v, gate_fold = r["left"], r["fold"], r["fold_v"], r["gate_fold"]
    qk, squares, square_parts = r["qk"], r["squares"], r["square_parts"]

    def fold_qk(i):
        embed, query, key = r[f"v_embed{i}"], r[f"v_query{i}"], r[f"v_key{i}"]
        loads[f"query{i}"].wait()
        loads[f"key{i}"].wait()
        landed(piece_copies[i])
        modul = jnp.sum(piece_parts[i].astype(f32), axis=0)
        line = lax.broadcasted_iota(jnp.int32, (16, some), 0)
        for q in range(4):
            at = slice(q * some, (q + 1) * some)
            shift, scale = modul[2 * q : 2 * q + 1], modul[2 * q + 1 : 2 * q + 2]
            left_ref[i, :kin, at] = (
                (embed[:, at].astype(f32) - means[i]) * (1.0 + scale)
            ).astype(bf16)
            shift_high, shift_low = split(shift)
            left_ref[i, kin:, at] = jnp.where(
                line == 0, shift_high.astype(f32), jnp.where(line == 1, shift_low.astype(f32), 0.0)
            ).astype(bf16)
        fold[i] = dot(left_ref[i], jnp.concatenate([query[...], key[...]], axis=1))

    def project_qk(i):
        folded = jnp.concatenate(split(fold[i, :kin].T), axis=1)
        tail = fold[i, kin : kin + 8].T
        offset = tail[:, :1] + tail[:, 1:2]
        for at in blocks:
            full = dot(folded, stack[:, at]) * rscale[i : i + 1, at] + offset
            qk[i, :, at] = full
            found = [full[j * head : (j + 1) * head] for j in range(2)]
            found = [jnp.sum(rows * rows, axis=0, keepdims=True) for rows in found]
            squares[i, :, at] = jnp.concatenate(found, axis=0).astype(squares.dtype)
        copies = exchange(
            "tm", n, lambda peer: squares.at[i], square_parts.at[i], sem(f"sums{i}")
        )
        square_parts[i, me] = squares[i]
        return copies

    values = r["values"]

    def fold_value(i):
        loads[f"value{i}"].wait()
        fold_v[i] = dot(left_ref[i], r[f"v_value{i}"][...])

    def fold_gate(i):
        out, proj = r[f"v_out{i}"], r[f"v_proj{i}"]
        loads[f"out{i}"].wait()
        gated = []
        for q in range(4):
            at = slice(q * some, (q + 1) * some)
            gate = gate_sum[2 * q + i : 2 * q + i + 1]
            gated.append((proj[:, at].astype(f32) * gate).astype(bf16))
        gate_fold[i] = dot_nt(out[...], jnp.concatenate(gated, axis=1))

    def join(i):
        gate_high, gate_low = split(gate_fold[i].T)
        value_high, value_low = split(fold_v[i])
        both = dot_nt(jnp.concatenate([gate_high, gate_low], axis=0), value_high)
        joint = both[:patch_rows] + both[patch_rows:] + dot_nt(gate_high, value_low)
        offset = joint[:, kin : kin + 1] + joint[:, kin + 1 : kin + 2]
        pairs = jnp.concatenate(split(joint[:, :kin]), axis=1)
        for at in blocks:
            full = dot(pairs, stack[:, at]) * rscale[i : i + 1, at] + offset
            values[i, :patch_rows, at] = full.astype(bf16)
            values[i, patch_rows:, at] = jnp.ones((16, block), bf16)

    fold_qk(0)
    landed(spread)
    for s in range(n):
        at = slice(s * frame, (s + 1) * frame)
        now = patches[s]
        before = patches[s - 1] if s else jnp.zeros_like(now)
        both = jnp.concatenate([now, before], axis=0)
        stack[:kin, at] = both
        stack[kin:, at] = both
    for i in (0, 1):
        gram_pair = jnp.concatenate(split(centered[i]), axis=1)
        for at in blocks:
            pair = stack[:, at]
            variance = jnp.sum(pair[:kin].astype(f32) * dot(gram_pair, pair), axis=0, keepdims=True)
            rscale[i : i + 1, at] = lax.rsqrt(jnp.maximum(variance, 0.0) + norm_floor)
    sums = [project_qk(0)]
    fold_value(0)
    fold_qk(1)
    sums.append(project_qk(1))
    fold_value(1)
    landed(piece_copies[2])
    gate_sum = jnp.sum(piece_parts[2].astype(f32), axis=0)
    fold_gate(0)
    fold_gate(1)
    join(0)
    join(1)

    groups = min(4, tokens // block)
    per_group = tokens // block // groups
    keys, terms, term_parts = r["keys"], r["terms"], r["term_parts"]

    starts = [block * b * (b + 1) // 2 for b in range(tokens // block)]

    def prepare(i):
        inverse = lax.rsqrt(
            jnp.sum(square_parts[i].astype(f32), axis=0) / (head * n) + norm_floor
        )
        gain = r[f"v_gain{i}"]
        gains = gain[0:1, :] * gain[1:2, :]
        to_query = math.log2(math.e) / math.sqrt(HD)
        for at in blocks:
            gained = qk[i, head:, at] * inverse[1:2, at]
            keys[i, at, :] = (gained.T * gains).astype(bf16)
            r["queries"][i, :, at] = (qk[i, :head, at] * (inverse[:1, at] * to_query)).astype(bf16)

    def put(i, b, powers, length):
        summed = dot(values[i, :, :length], powers)
        term = (summed[:patch_rows] / summed[patch_rows : patch_rows + 1]).astype(bf16)
        for j in range(2):
            terms[i, 2 * b + j] = term[:, j * frame : (j + 1) * frame]

    def score(i):
        early = lax.broadcasted_iota(jnp.int32, (frame, block), 1) < frame
        for b, (at, start) in enumerate(zip(blocks, starts)):
            length = (b + 1) * block
            scores = dot(keys[i, :length], r["queries"][i, :, at])
            r["scores"][i, start : start + length - frame] = scores[: length - frame]
            edge = jnp.where(early, -1e30, scores[length - frame :])
            r["scores"][i, start + length - frame : start + length] = edge

    def soften(i):
        for b, start in enumerate(starts):
            rows = slice(start, start + (b + 1) * block)
            peak = jnp.max(r["scores"][i, rows], axis=0, keepdims=True)
            r["powers"][i, rows] = jnp.exp2(r["scores"][i, rows] - peak).astype(bf16)

    def combine(i):
        for b, start in enumerate(starts):
            length = (b + 1) * block
            put(i, b, r["powers"][i, start : start + length], length)

    def looped(i):
        for group in range(groups):
            length = (group + 1) * per_group * block
            low = length - per_group * block

            def block_step(b, carry):
                at = pl.ds(pl.multiple_of(b * block, block), block)
                scores = dot(keys[i, :length], r["queries"][i, :, at])
                shape = (length - low, block)
                key_frame = (lax.broadcasted_iota(jnp.int32, shape, 0) + low) // frame
                query_frame = (lax.broadcasted_iota(jnp.int32, shape, 1) + b * block) // frame
                edge = jnp.where(key_frame <= query_frame, scores[low:], -1e30)
                scores = jnp.concatenate([scores[:low], edge], axis=0) if low else edge
                peak = jnp.max(scores, axis=0, keepdims=True)
                put(i, b, jnp.exp2(scores - peak).astype(bf16), length)
                return carry

            lax.fori_loop(group * per_group, (group + 1) * per_group, block_step, 0)

    def hand_out(i):
        copies = exchange(
            "tm", n, lambda peer: terms.at[i, peer], term_parts.at[i], sem(f"give{i}")
        )
        term_parts[i, me] = terms[i, me]
        return copies

    for name in ("gain0", "gain1"):
        loads[name].wait()
    give = []
    for i in (0, 1):
        landed(sums[i])
        prepare(i)
        if per_group == 1:
            score(i)
            soften(i)
            combine(i)
        else:
            looped(i)
        give.append(hand_out(i))

    own = stack[:, pl.ds(pl.multiple_of(me * frame, frame), frame)]
    velocity = []
    for i in (0, 1):
        inner = jnp.concatenate(split(gram[i, kin:extra]), axis=1)
        velocity.append(dot(inner, own))
    for i in (0, 1):
        landed(give[i])
        velocity[i] = velocity[i] + jnp.sum(term_parts[i].astype(f32), axis=0)
    pred_real = noisy - level * velocity[0]
    pred_fake = noisy - level * velocity[1]
    difference = pred_fake - pred_real
    rounded, rounded_other, gap, gaps = r["rounded"], r["rounded_other"], r["gap"], r["gaps"]
    rounded[...] = difference.astype(bf16)
    swap = send("swap", rounded, rounded_other, 0, other)
    swap.start()
    distance = jnp.abs(made - pred_real)
    distance = jnp.sum(jnp.sum(distance, axis=0, keepdims=True), axis=1, keepdims=True)
    gap[...] = jnp.broadcast_to(distance, gap.shape)
    gap_copies = exchange("tm", n, lambda peer: gap, gaps, sem("gap"))
    gaps[me] = gap[...]
    products, partial, gathered = r["products"], r["partial"], r["gathered"]
    hops = [*range(chips - 1, 0, -1), 0]
    for hop in hops:
        products[hop] = dot(rounded[...], hidden[:, part_of(partner(chip, hop, chips), core)])
    all_held = send("held", held, held, 0, other)
    all_held.wait_recv()
    swap.wait_recv()
    order = [*range(nb - 1, 0, -1), 0]
    for hop in hops:
        at = partner(chip, hop, chips)
        whole = products[hop] + dot(rounded_other[...], held[at])
        partial[hop] = whole.reshape(partial.shape[1:]).astype(bf16)
    for k in order:
        piece = partner(mine, k, nb)
        for hop in hops[:-1]:
            where = {"tm": 2 * partner(chip, hop, chips) + core}
            send("plane", partial.at[hop, piece], gathered.at[k, hop], k, where).start()
    landed(gap_copies)
    normalizer = jnp.maximum(jnp.sum(gaps[...], axis=0) / (patch_rows * tokens), gap_floor)
    r["difference"][...] = difference / normalizer[:1, :1]
    factor = 1.0 / (normalizer[:1, :1] * math.sqrt(nb * tokens))
    mixed, quarters, merged, grad = r["mixed"], r["quarters"], r["merged"], r["grad"]
    for k in order:
        piece = partner(mine, k, nb)
        near = gathered.at[k, pl.ds(1, chips - 1)]
        send("plane", near, near, k, other).wait_recv()
        summed = partial[0, piece].astype(f32)
        for hop in hops[:-1]:
            summed = summed + gathered[k, hop].astype(f32)
        summed = (summed * factor).astype(bf16)
        if k:
            mixed[k] = summed
            send("across", mixed.at[k], quarters.at[k], 0, {"batch": piece}).start()
        else:
            quarters[0] = summed
    far = quarters.at[pl.ds(1, nb - 1)]
    across = send("across", far, far, 0, other)
    across.wait_recv()
    merged[mine] = jnp.sum(quarters[...].astype(f32), axis=0).astype(bf16)
    grad[core, chip, mine] = merged[mine]
    back = []
    for k in range(1, nb):
        back.append(
            send("back", merged.at[mine], merged.at[mine], k, {"batch": partner(mine, k, nb)})
        )
        back[-1].start()

    def to_chips(piece):
        for hop in range(1, chips):
            where = {"tm": 2 * partner(chip, hop, chips) + core}
            send("chain", merged.at[piece], grad.at[core, chip, piece], hop, where).start()

    to_chips(mine)
    for k in range(1, nb):
        back[k - 1].wait_recv()
        piece = partner(mine, k, nb)
        grad[core, chip, piece] = merged[piece]
        to_chips(piece)

    def to_partner(at):
        send("share", grad.at[core, at], grad.at[core, at], 0, other).start()

    to_partner(chip)
    for hop in range(1, chips):
        at = partner(chip, hop, chips)
        send("chain", grad.at[core, at], grad.at[core, at], hop, other).wait_recv()
        to_partner(at)
    whole = send("share", grad.at[core], grad.at[1 - core], 0, other)
    whole.wait_recv()
    for copies in (
        *piece_copies, spread, *sums, *give, gap_copies,
    ):
        gone(copies)
    all_held.wait_send()
    swap.wait_send()
    for k in order:
        near = gathered.at[k, pl.ds(1, chips - 1)]
        send("plane", near, near, k, other).wait_send()
    across.wait_send()
    rest = merged.at[pl.ds(0, nb - 1)]
    send("back", rest, rest, 0, other).wait_send()
    for hop in range(1, chips):
        send("chain", merged, merged, 0, other).wait_send()
    whole.wait_send()


def last_kernel(part, grad_ref, difference_ref, weight_out, difference_out, wide_ref, sems):
    patch_rows, width = wide_ref.shape
    copies = [pltpu.make_async_copy(difference_ref, difference_out, sems.at[0])]
    copies[0].start()
    for s in range(width // part):
        at = slice(s * part, (s + 1) * part)
        wide_ref[:, at] = grad_ref[s % 2, s // 2].reshape(patch_rows, part).astype(f32)
        copies.append(
            pltpu.make_async_copy(wide_ref.at[:, at], weight_out.at[:, at], sems.at[s + 1])
        )
        copies[-1].start()
    for copy in copies:
        copy.wait()


def per_device(
    hidden_states,
    gen_weight,
    noise_field,
    timesteps,
    embed_real,
    time_real,
    query_real,
    key_real,
    value_real,
    out_real,
    gain_real,
    proj_real,
    embed_fake,
    time_fake,
    query_fake,
    key_fake,
    value_fake,
    out_fake,
    gain_fake,
    proj_fake,
):
    n = lax.axis_size("tm")
    nb = lax.axis_size("batch")
    frame = hidden_states.shape[1]
    tokens = frame * n
    patch_rows, width = gen_weight.shape
    part = -(-width // (n * 128)) * 128
    while width % part:
        part += 128
    chunks = width // part
    many = tokens // (2 * frame)
    held_rows = many * (many + 1) * frame if many <= 4 else 16
    chips, quarter, head = n // 2, patch_rows // nb, query_real.shape[1]
    kin = 2 * patch_rows
    inputs = dict(
        time0=time_real.transpose(1, 0, 2), time1=time_fake.transpose(1, 0, 2),
        hidden=hidden_states[0], gen=gen_weight, noise=noise_field[0],
        embed0=embed_real, proj0=proj_real, embed1=embed_fake, proj1=proj_fake,
        query0=query_real, key0=key_real, query1=query_fake, key1=key_fake,
        value0=value_real, out0=out_real, value1=value_fake, out1=out_fake,
        gain0=gain_real, gain1=gain_fake,
    )
    vm = pltpu.VMEM
    outputs = dict(
        difference=vm((patch_rows, frame), f32),
        grad=vm((2, chips, nb, quarter, part), bf16),
    )
    scratch = {}
    for name in LOADS:
        array = inputs[name]
        scratch["v_" + name] = vm(array.shape, array.dtype)
    scratch.update(
        load_sem=pltpu.SemaphoreType.DMA((len(LOADS),)),
        patches=vm((n, patch_rows, frame), bf16),
        pieces=vm((3, 8, width // 4), bf16),
        piece_parts=vm((3, n, 8, width // 4), bf16),
        noisy=vm((patch_rows, frame), bf16),
        held=vm((chips, frame, part), bf16),
        products=vm((chips, patch_rows, part), f32),
        partial=vm((chips, nb, quarter, part), bf16),
        gathered=vm((nb, chips, quarter, part), bf16),
        gram=vm((2, kin + patch_rows + 16, kin), f32),
        stack=vm((2 * kin, tokens), bf16),
        rscale=vm((2, tokens), f32),
        left=vm((2, kin + 16, width), bf16),
        fold=vm((2, kin + 16, 2 * head), f32),
        fold_v=vm((2, kin + 16, head), f32),
        gate_fold=vm((2, head, patch_rows), f32),
        qk=vm((2, 2 * head, tokens), f32),
        squares=vm((2, 2, tokens), bf16),
        square_parts=vm((2, n, 2, tokens), bf16),
        values=vm((2, patch_rows + 16, tokens), bf16),
        keys=vm((2, tokens, head), bf16),
        queries=vm((2, head, tokens), bf16),
        scores=vm((2, held_rows, 2 * frame), f32),
        powers=vm((2, held_rows, 2 * frame), bf16),
        terms=vm((2, n, patch_rows, frame), bf16),
        term_parts=vm((2, n, patch_rows, frame), bf16),
        gap=vm((8, 128), f32),
        gaps=vm((n, 8, 128), f32),
        rounded=vm((patch_rows, frame), bf16),
        rounded_other=vm((patch_rows, frame), bf16),
        mixed=vm((nb, quarter, part), bf16),
        quarters=vm((nb, quarter, part), bf16),
        merged=vm((nb, quarter, part), bf16),
    )
    for name, count in dict(
        piece0=1, piece1=1, piece2=1, spread=1, sums0=1, sums1=1, give0=1, give1=1, gap=1,
        held=1, swap=1, plane=nb, across=1, back=nb, chain=chips, share=1,
    ).items():
        scratch["s_" + name] = pltpu.SemaphoreType.DMA((1,))
        scratch["r_" + name] = pltpu.SemaphoreType.DMA((count,))
    names = ("timesteps", *LOADS, *outputs, *scratch)
    difference, grad = pl.pallas_call(
        functools.partial(main_kernel, n, nb, part, names),
        out_shape=list(outputs.values()),
        in_specs=[pl.BlockSpec(memory_space=pltpu.SMEM)]
        + [pl.BlockSpec(memory_space=pltpu.HBM)] * len(LOADS),
        out_specs=[pl.BlockSpec(memory_space=pltpu.VMEM)] * 2,
        scratch_shapes=list(scratch.values()),
        compiler_params=pltpu.CompilerParams(
            collective_id=0, has_side_effects=True, vmem_limit_bytes=60 * 1024 * 1024
        ),
    )(timesteps, *(pltpu.with_memory_space_constraint(inputs[x], pltpu.HBM) for x in LOADS))
    weight_grad, difference = pl.pallas_call(
        functools.partial(last_kernel, part),
        out_shape=[
            jax.ShapeDtypeStruct((patch_rows, width), f32),
            jax.ShapeDtypeStruct((patch_rows, frame), f32),
        ],
        in_specs=[pl.BlockSpec(memory_space=pltpu.VMEM)] * 2,
        out_specs=[pl.BlockSpec(memory_space=pl.ANY)] * 2,
        scratch_shapes=[vm((patch_rows, width), f32), pltpu.SemaphoreType.DMA((chunks + 1,))],
        compiler_params=pltpu.CompilerParams(vmem_limit_bytes=8 * 1024 * 1024),
    )(*(pltpu.with_memory_space_constraint(x, pltpu.VMEM) for x in (grad, difference)))
    return (difference[None], weight_grad)


def solution(mesh):
    in_specs = (
        P("batch", "tm", None),
        P(),
        P("batch", None, "tm"),
        P("batch"),
        P(),
        P("tm", None, None),
        P(None, "tm"),
        P(None, "tm"),
        P(None, "tm"),
        P("tm", None),
        P(None, "tm"),
        P(),
        P(),
        P("tm", None, None),
        P(None, "tm"),
        P(None, "tm"),
        P(None, "tm"),
        P("tm", None),
        P(None, "tm"),
        P(),
    )
    out_specs = (P("batch", None, "tm"), P())
    return jax.shard_map(
        per_device, mesh=mesh, in_specs=in_specs, out_specs=out_specs, check_vma=False
    )
```

```python
import functools
import math

import jax
import jax.numpy as jnp
from jax import lax
from jax.experimental import pallas as pl
from jax.experimental.pallas import tpu as pltpu
from jax.sharding import PartitionSpec as P

HD = 128
FREQ = 256

norm_floor = 0.05
gap_floor = 0.25

MESH = pl.DeviceIdType.MESH
f32 = jnp.float32
bf16 = jnp.bfloat16


def hail(sizes):
    barrier = pltpu.get_barrier_semaphore()
    for axis, size in sizes.items():
        me = lax.axis_index(axis)
        for k in range(1, size):
            pl.semaphore_signal(
                barrier, inc=1, device_id={axis: lax.rem(me + k, size)}, device_id_type=MESH
            )


def meet(sizes):
    count = sum(size - 1 for size in sizes.values())
    pl.semaphore_wait(pltpu.get_barrier_semaphore(), count)


def partner(me, k, size):
    if size & (size - 1):
        return lax.rem(me + k, size)
    peer, bit = me, 1
    while bit < size:
        if k & bit:
            peer = peer + bit - 2 * bit * lax.rem(lax.div(me, bit), 2)
        bit *= 2
    return peer


class Exchange:
    def __init__(self, axis, size, source, slots, sems):
        self.axis, self.size, self.source, self.slots, self.sems = axis, size, source, slots, sems

    def start(self):
        me = lax.axis_index(self.axis)
        for k in range(self.size - 1, 0, -1):
            peer = partner(me, k, self.size)
            self.copy(self.source(peer), self.slots.at[me], peer).start()
        return self

    def copy(self, source, target, peer):
        return pltpu.make_async_remote_copy(
            src_ref=source,
            dst_ref=target,
            send_sem=self.sems[0].at[0],
            recv_sem=self.sems[1].at[0],
            device_id={self.axis: peer},
            device_id_type=MESH,
        )

    def all(self):
        both = self.slots.at[pl.ds(0, self.size - 1)]
        return self.copy(both, both, lax.axis_index(self.axis))


def exchange(axis, size, source, slots, sems):
    return Exchange(axis, size, source, slots, sems).start()


def landed(copies):
    copies.all().wait_recv()


def gone(copies):
    copies.all().wait_send()


def split(wide):
    high = wide.astype(bf16)
    return high, (wide - high.astype(f32)).astype(bf16)


def dot_nt(left, right):
    return lax.dot_general(left, right, (((1,), (1,)), ((), ())), preferred_element_type=f32)


def dot(left, right):
    return jnp.dot(left, right, preferred_element_type=f32)


LOADS = (
    "time0", "time1", "hidden", "gen", "noise", "embed0", "proj0", "embed1",
    "proj1", "query0", "key0", "query1", "key1", "value0", "out0", "value1", "out1", "gain0", "gain1",
)


def main_kernel(n, nb, part, names, *refs):
    r = dict(zip(names, refs, strict=True))
    me = lax.axis_index("tm")
    mine = lax.axis_index("batch")
    core, chip = lax.rem(me, 2), lax.div(me, 2)
    chips = n // 2
    hidden, stack = r["v_hidden"], r["stack"]
    noisy_ref = r["noisy"]
    patch_rows, frame = noisy_ref.shape
    tokens = n * frame
    kin = 2 * patch_rows
    width = hidden.shape[1]
    chunks = width // part
    head = r["v_query0"].shape[1]
    freq_rows = r["v_time0"].shape[1]
    loads = {}
    for i, name in enumerate(LOADS):
        loads[name] = pltpu.make_async_copy(r[name], r["v_" + name], r["load_sem"].at[i])
        loads[name].start()
    hail({"tm": n, "batch": nb})

    def sem(name):
        return r["s_" + name], r["r_" + name]

    half = FREQ // 2
    time_step = jnp.full((16, half), r["timesteps"][0], jnp.int32).astype(f32)
    place = lax.broadcasted_iota(jnp.int32, (16, half), 1)
    angles = time_step
    bit = 1
    while bit < half:
        factor = math.exp(-math.log(10000.0) * bit / half)
        angles = angles * jnp.where(lax.rem(lax.div(place, bit), 2) == 1, factor, 1.0)
        bit *= 2
    wave = jnp.concatenate([jnp.cos(angles), jnp.sin(angles)], axis=1).astype(bf16)
    raw = time_step[:8] * (1.0 / 1000.0)
    level = ((5.0 * raw) / (1.0 + 4.0 * raw))[:1, :1]
    picked = (2 * half, 3 * freq_rows)
    column = lax.rem(lax.broadcasted_iota(jnp.int32, picked, 1), freq_rows) + me * freq_rows
    chosen = (lax.broadcasted_iota(jnp.int32, picked, 0) == column).astype(f32).astype(bf16)
    own_wave = dot(wave, chosen)
    own_wave = jnp.concatenate([own_wave, own_wave], axis=0)
    block_of = lax.broadcasted_iota(jnp.int32, own_wave.shape, 1) // freq_rows
    row_of = lax.broadcasted_iota(jnp.int32, own_wave.shape, 0)
    share = None
    for i in (0, 1):
        loads[f"time{i}"].wait()
        table = r[f"v_time{i}"]
        early = (row_of // 8 == i) & (lax.rem(row_of, 2) == block_of)
        late = (row_of // 8 == 2) & (lax.rem(row_of, 2) == i) & (block_of == 2)
        left = jnp.where(early | late, own_wave, 0.0).astype(bf16)
        if freq_rows % 16:
            for j in range(3):
                term = dot(left[:, j * freq_rows : (j + 1) * freq_rows], table[j])
                share = term if share is None else share + term
        else:
            term = dot(left, table[...].reshape(3 * freq_rows, width))
            share = term if share is None else share + term
    pieces, piece_parts = r["pieces"], r["piece_parts"]
    some = width // 4
    line = lax.broadcasted_iota(jnp.int32, (8, some), 0) // 2
    for g in range(3):
        rows = share[8 * g : 8 * g + 8]
        picked = rows[:, :some]
        for q in range(1, 4):
            picked = jnp.where(line == q, rows[:, q * some : (q + 1) * some], picked)
        pieces[g] = picked.astype(bf16)
    meet({"tm": n, "batch": nb})

    def hand_on(g):
        copies = exchange("tm", n, lambda peer: pieces.at[g], piece_parts.at[g], sem(f"piece{g}"))
        piece_parts[g, me] = pieces[g]
        return copies

    piece_copies = [hand_on(0)]

    loads["hidden"].wait()
    loads["gen"].wait()
    loads["noise"].wait()
    made = dot_nt(hidden[...], r["v_gen"][...]).T.astype(bf16).astype(f32)
    noisy = ((1.0 - level) * made + level * r["v_noise"][...].astype(f32)).astype(bf16)
    noisy_ref[...] = noisy
    patches = r["patches"]
    spread = exchange("tm", n, lambda peer: noisy_ref, patches, sem("spread"))
    patches[me] = noisy_ref[...]
    piece_copies.extend([hand_on(1), hand_on(2)])
    noisy = noisy.astype(f32)

    def columns(s):
        return pl.ds(pl.multiple_of(s * part, 128), part)

    held = r["held"]
    other = {"tm": me + 1 - 2 * core}

    def send(name, source, target, at, where, slot=0):
        return pltpu.make_async_remote_copy(
            src_ref=source,
            dst_ref=target,
            send_sem=r["s_" + name].at[slot],
            recv_sem=r["r_" + name].at[at],
            device_id=where,
            device_id_type=MESH,
        )

    def part_of(q, side):
        return columns(lax.rem(2 * q + side, chunks))

    gram = r["gram"]
    extra = kin + patch_rows

    def gram_of(i):
        embed, proj = r[f"v_embed{i}"], r[f"v_proj{i}"]
        loads[f"embed{i}"].wait()
        loads[f"proj{i}"].wait()
        ones = jnp.ones((16, width), bf16)
        gram[i] = dot_nt(jnp.concatenate([embed[...], proj[...], ones], axis=0), embed[...])

    gram_of(0)
    for q in range(chips):
        send("held", hidden.at[:, part_of(q, 1 - core)], held.at[q], 0, other).start()
    gram_of(1)

    block = 2 * frame
    blocks = [slice(s * block, (s + 1) * block) for s in range(tokens // block)]
    rscale = r["rscale"]
    means, centered = [], []
    for i in (0, 1):
        mean_row = gram[i, extra : extra + 8] / width
        means.append(mean_row.T[:, :1])
        centered.append(gram[i, :kin] / width - means[i] * mean_row[:1])

    left_ref, fold, fold_v, gate_fold = r["left"], r["fold"], r["fold_v"], r["gate_fold"]
    qk, squares, square_parts = r["qk"], r["squares"], r["square_parts"]

    def fold_qk(i):
        embed, query, key = r[f"v_embed{i}"], r[f"v_query{i}"], r[f"v_key{i}"]
        landed(piece_copies[i])
        modul = jnp.sum(piece_parts[i].astype(f32), axis=0)
        line = lax.broadcasted_iota(jnp.int32, (16, some), 0)
        for q in range(4):
            at = slice(q * some, (q + 1) * some)
            shift, scale = modul[2 * q : 2 * q + 1], modul[2 * q + 1 : 2 * q + 2]
            left_ref[i, :kin, at] = (
                (embed[:, at].astype(f32) - means[i]) * (1.0 + scale)
            ).astype(bf16)
            shift_high, shift_low = split(shift)
            left_ref[i, kin:, at] = jnp.where(
                line == 0, shift_high.astype(f32), jnp.where(line == 1, shift_low.astype(f32), 0.0)
            ).astype(bf16)
        fold[i] = dot(left_ref[i], jnp.concatenate([query[...], key[...]], axis=1))

    def project_qk(i):
        folded = jnp.concatenate(split(fold[i, :kin].T), axis=1)
        tail = fold[i, kin : kin + 8].T
        offset = tail[:, :1] + tail[:, 1:2]
        for at in blocks:
            full = dot(folded, stack[:, at]) * rscale[i : i + 1, at] + offset
            qk[i, :, at] = full
            found = [full[j * head : (j + 1) * head] for j in range(2)]
            found = [jnp.sum(rows * rows, axis=0, keepdims=True) for rows in found]
            squares[i, :, at] = jnp.concatenate(found, axis=0).astype(squares.dtype)
        copies = exchange(
            "tm", n, lambda peer: squares.at[i], square_parts.at[i], sem(f"sums{i}")
        )
        square_parts[i, me] = squares[i]
        return copies

    values = r["values"]

    def fold_value(i):
        fold_v[i] = dot(left_ref[i], r[f"v_value{i}"][...])

    def fold_gate(i):
        out, proj = r[f"v_out{i}"], r[f"v_proj{i}"]
        gated = []
        for q in range(4):
            at = slice(q * some, (q + 1) * some)
            gate = gate_sum[2 * q + i : 2 * q + i + 1]
            gated.append((proj[:, at].astype(f32) * gate).astype(bf16))
        gate_fold[i] = dot_nt(out[...], jnp.concatenate(gated, axis=1))

    def join(i):
        gate_high, gate_low = split(gate_fold[i].T)
        value_high, value_low = split(fold_v[i])
        both = dot_nt(jnp.concatenate([gate_high, gate_low], axis=0), value_high)
        joint = both[:patch_rows] + both[patch_rows:] + dot_nt(gate_high, value_low)
        offset = joint[:, kin : kin + 1] + joint[:, kin + 1 : kin + 2]
        pairs = jnp.concatenate(split(joint[:, :kin]), axis=1)
        for at in blocks:
            full = dot(pairs, stack[:, at]) * rscale[i : i + 1, at] + offset
            values[i, :patch_rows, at] = full.astype(bf16)
            values[i, patch_rows:, at] = jnp.ones((16, block), bf16)

    loads["query0"].wait()
    loads["key0"].wait()
    fold_qk(0)
    for name in LOADS[LOADS.index("query1") :]:
        loads[name].wait()
    landed(spread)
    for s in range(n):
        at = slice(s * frame, (s + 1) * frame)
        now = patches[s]
        before = patches[s - 1] if s else jnp.zeros_like(now)
        both = jnp.concatenate([now, before], axis=0)
        stack[:kin, at] = both
        stack[kin:, at] = both
    for i in (0, 1):
        gram_pair = jnp.concatenate(split(centered[i]), axis=1)
        for at in blocks:
            pair = stack[:, at]
            variance = jnp.sum(pair[:kin].astype(f32) * dot(gram_pair, pair), axis=0, keepdims=True)
            rscale[i : i + 1, at] = lax.rsqrt(jnp.maximum(variance, 0.0) + norm_floor)
    sums = [project_qk(0)]
    fold_value(0)
    fold_qk(1)
    sums.append(project_qk(1))
    fold_value(1)
    landed(piece_copies[2])
    gate_sum = jnp.sum(piece_parts[2].astype(f32), axis=0)
    fold_gate(0)
    fold_gate(1)
    join(0)
    join(1)

    groups = min(4, tokens // block)
    per_group = tokens // block // groups
    keys, terms, term_parts = r["keys"], r["terms"], r["term_parts"]

    starts = [block * b * (b + 1) // 2 for b in range(tokens // block)]

    def prepare(i):
        inverse = lax.rsqrt(
            jnp.sum(square_parts[i].astype(f32), axis=0) / (head * n) + norm_floor
        )
        gain = r[f"v_gain{i}"]
        gains = gain[0:1, :] * gain[1:2, :]
        to_query = math.log2(math.e) / math.sqrt(HD)
        for at in blocks:
            gained = qk[i, head:, at] * inverse[1:2, at]
            keys[i, at, :] = (gained.T * gains).astype(bf16)
            r["queries"][i, :, at] = (qk[i, :head, at] * (inverse[:1, at] * to_query)).astype(bf16)

    def put(i, b, powers, length):
        summed = dot(values[i, :, :length], powers)
        term = (summed[:patch_rows] / summed[patch_rows : patch_rows + 1]).astype(bf16)
        for j in range(2):
            terms[i, 2 * b + j] = term[:, j * frame : (j + 1) * frame]

    def score(i):
        early = lax.broadcasted_iota(jnp.int32, (frame, block), 1) < frame
        for b, (at, start) in enumerate(zip(blocks, starts)):
            length = (b + 1) * block
            scores = dot(keys[i, :length], r["queries"][i, :, at])
            r["scores"][i, start : start + length - frame] = scores[: length - frame]
            edge = jnp.where(early, -1e30, scores[length - frame :])
            r["scores"][i, start + length - frame : start + length] = edge

    def soften(i):
        for b, start in enumerate(starts):
            rows = slice(start, start + (b + 1) * block)
            peak = jnp.max(r["scores"][i, rows], axis=0, keepdims=True)
            r["powers"][i, rows] = jnp.exp2(r["scores"][i, rows] - peak).astype(bf16)

    def combine(i):
        for b, start in enumerate(starts):
            length = (b + 1) * block
            put(i, b, r["powers"][i, start : start + length], length)

    def looped(i):
        for group in range(groups):
            length = (group + 1) * per_group * block
            low = length - per_group * block

            def block_step(b, carry):
                at = pl.ds(pl.multiple_of(b * block, block), block)
                scores = dot(keys[i, :length], r["queries"][i, :, at])
                shape = (length - low, block)
                key_frame = (lax.broadcasted_iota(jnp.int32, shape, 0) + low) // frame
                query_frame = (lax.broadcasted_iota(jnp.int32, shape, 1) + b * block) // frame
                edge = jnp.where(key_frame <= query_frame, scores[low:], -1e30)
                scores = jnp.concatenate([scores[:low], edge], axis=0) if low else edge
                peak = jnp.max(scores, axis=0, keepdims=True)
                put(i, b, jnp.exp2(scores - peak).astype(bf16), length)
                return carry

            lax.fori_loop(group * per_group, (group + 1) * per_group, block_step, 0)

    def hand_out(i):
        copies = exchange(
            "tm", n, lambda peer: terms.at[i, peer], term_parts.at[i], sem(f"give{i}")
        )
        term_parts[i, me] = terms[i, me]
        return copies

    give = []
    for i in (0, 1):
        landed(sums[i])
        prepare(i)
        if per_group == 1:
            score(i)
            soften(i)
            combine(i)
        else:
            looped(i)
        give.append(hand_out(i))

    own = stack[:, pl.ds(pl.multiple_of(me * frame, frame), frame)]
    velocity = []
    for i in (0, 1):
        inner = jnp.concatenate(split(gram[i, kin:extra]), axis=1)
        velocity.append(dot(inner, own))
    for i in (0, 1):
        landed(give[i])
        velocity[i] = velocity[i] + jnp.sum(term_parts[i].astype(f32), axis=0)
    pred_real = noisy - level * velocity[0]
    pred_fake = noisy - level * velocity[1]
    difference = pred_fake - pred_real
    rounded, rounded_other, gap, gaps = r["rounded"], r["rounded_other"], r["gap"], r["gaps"]
    rounded[...] = difference.astype(bf16)
    swap = send("swap", rounded, rounded_other, 0, other)
    swap.start()
    distance = jnp.abs(made - pred_real)
    distance = jnp.sum(jnp.sum(distance, axis=0, keepdims=True), axis=1, keepdims=True)
    gap[...] = jnp.broadcast_to(distance, gap.shape)
    gap_copies = exchange("tm", n, lambda peer: gap, gaps, sem("gap"))
    gaps[me] = gap[...]
    products, partial, gathered = r["products"], r["partial"], r["gathered"]
    hops = [*range(chips - 1, 0, -1), 0]
    for hop in hops:
        products[hop] = dot(rounded[...], hidden[:, part_of(partner(chip, hop, chips), core)])
    all_held = send("held", held, held, 0, other)
    all_held.wait_recv()
    swap.wait_recv()
    order = [*range(nb - 1, 0, -1), 0]
    for hop in hops:
        at = partner(chip, hop, chips)
        whole = products[hop] + dot(rounded_other[...], held[at])
        partial[hop] = whole.reshape(partial.shape[1:]).astype(bf16)
    for k in order:
        piece = partner(mine, k, nb)
        for hop in hops[:-1]:
            where = {"tm": 2 * partner(chip, hop, chips) + core}
            send("plane", partial.at[hop, piece], gathered.at[k, hop], k, where).start()
    landed(gap_copies)
    normalizer = jnp.maximum(jnp.sum(gaps[...], axis=0) / (patch_rows * tokens), gap_floor)
    r["difference"][...] = difference / normalizer[:1, :1]
    factor = 1.0 / (normalizer[:1, :1] * math.sqrt(nb * tokens))
    mixed, quarters, merged, grad = r["mixed"], r["quarters"], r["merged"], r["grad"]
    for k in order:
        piece = partner(mine, k, nb)
        near = gathered.at[k, pl.ds(1, chips - 1)]
        send("plane", near, near, k, other).wait_recv()
        summed = partial[0, piece].astype(f32)
        for hop in hops[:-1]:
            summed = summed + gathered[k, hop].astype(f32)
        summed = (summed * factor).astype(bf16)
        if k:
            mixed[k] = summed
            send("across", mixed.at[k], quarters.at[k], 0, {"batch": piece}).start()
        else:
            quarters[0] = summed
    far = quarters.at[pl.ds(1, nb - 1)]
    across = send("across", far, far, 0, other)
    across.wait_recv()
    merged[mine] = jnp.sum(quarters[...].astype(f32), axis=0).astype(bf16)
    grad[core, chip, mine] = merged[mine]
    back = []
    for k in range(1, nb):
        back.append(
            send("back", merged.at[mine], merged.at[mine], k, {"batch": partner(mine, k, nb)})
        )

    for copy in back[::-1]:
        copy.start()

    def to_chips(piece):
        for hop in range(chips - 1, 0, -1):
            where = {"tm": 2 * partner(chip, hop, chips) + core}
            send("chain", merged.at[piece], grad.at[core, chip, piece], hop, where).start()

    to_chips(mine)
    for k in range(1, nb):
        back[k - 1].wait_recv()
        piece = partner(mine, k, nb)
        grad[core, chip, piece] = merged[piece]
        to_chips(piece)

    def to_partner(at):
        send("share", grad.at[core, at], grad.at[core, at], 0, other).start()

    to_partner(chip)
    for hop in range(1, chips):
        at = partner(chip, hop, chips)
        send("chain", grad.at[core, at], grad.at[core, at], hop, other).wait_recv()
        to_partner(at)
    whole = send("share", grad.at[core], grad.at[1 - core], 0, other)
    whole.wait_recv()
    for copies in (
        *piece_copies, spread, *sums, *give, gap_copies,
    ):
        gone(copies)
    all_held.wait_send()
    swap.wait_send()
    for k in order:
        near = gathered.at[k, pl.ds(1, chips - 1)]
        send("plane", near, near, k, other).wait_send()
    across.wait_send()
    rest = merged.at[pl.ds(0, nb - 1)]
    send("back", rest, rest, 0, other).wait_send()
    for hop in range(1, chips):
        send("chain", merged, merged, 0, other).wait_send()
    whole.wait_send()


def last_kernel(part, grad_ref, difference_ref, weight_out, difference_out, wide_ref, sems):
    patch_rows, width = wide_ref.shape
    copies = [pltpu.make_async_copy(difference_ref, difference_out, sems.at[0])]
    copies[0].start()
    for s in range(width // part):
        at = slice(s * part, (s + 1) * part)
        wide_ref[:, at] = grad_ref[s % 2, s // 2].reshape(patch_rows, part).astype(f32)
        copies.append(
            pltpu.make_async_copy(wide_ref.at[:, at], weight_out.at[:, at], sems.at[s + 1])
        )
        copies[-1].start()
    for copy in copies:
        copy.wait()


def per_device(
    hidden_states,
    gen_weight,
    noise_field,
    timesteps,
    embed_real,
    time_real,
    query_real,
    key_real,
    value_real,
    out_real,
    gain_real,
    proj_real,
    embed_fake,
    time_fake,
    query_fake,
    key_fake,
    value_fake,
    out_fake,
    gain_fake,
    proj_fake,
):
    n = lax.axis_size("tm")
    nb = lax.axis_size("batch")
    frame = hidden_states.shape[1]
    tokens = frame * n
    patch_rows, width = gen_weight.shape
    part = -(-width // (n * 128)) * 128
    while width % part:
        part += 128
    chunks = width // part
    many = tokens // (2 * frame)
    held_rows = many * (many + 1) * frame if many <= 4 else 16
    chips, quarter, head = n // 2, patch_rows // nb, query_real.shape[1]
    kin = 2 * patch_rows
    inputs = dict(
        time0=time_real.transpose(1, 0, 2), time1=time_fake.transpose(1, 0, 2),
        hidden=hidden_states[0], gen=gen_weight, noise=noise_field[0],
        embed0=embed_real, proj0=proj_real, embed1=embed_fake, proj1=proj_fake,
        query0=query_real, key0=key_real, query1=query_fake, key1=key_fake,
        value0=value_real, out0=out_real, value1=value_fake, out1=out_fake,
        gain0=gain_real, gain1=gain_fake,
    )
    vm = pltpu.VMEM
    outputs = dict(
        difference=vm((patch_rows, frame), f32),
        grad=vm((2, chips, nb, quarter, part), bf16),
    )
    scratch = {}
    for name in LOADS:
        array = inputs[name]
        scratch["v_" + name] = vm(array.shape, array.dtype)
    scratch.update(
        load_sem=pltpu.SemaphoreType.DMA((len(LOADS),)),
        patches=vm((n, patch_rows, frame), bf16),
        pieces=vm((3, 8, width // 4), bf16),
        piece_parts=vm((3, n, 8, width // 4), bf16),
        noisy=vm((patch_rows, frame), bf16),
        held=vm((chips, frame, part), bf16),
        products=vm((chips, patch_rows, part), f32),
        partial=vm((chips, nb, quarter, part), bf16),
        gathered=vm((nb, chips, quarter, part), bf16),
        gram=vm((2, kin + patch_rows + 16, kin), f32),
        stack=vm((2 * kin, tokens), bf16),
        rscale=vm((2, tokens), f32),
        left=vm((2, kin + 16, width), bf16),
        fold=vm((2, kin + 16, 2 * head), f32),
        fold_v=vm((2, kin + 16, head), f32),
        gate_fold=vm((2, head, patch_rows), f32),
        qk=vm((2, 2 * head, tokens), f32),
        squares=vm((2, 2, tokens), bf16),
        square_parts=vm((2, n, 2, tokens), bf16),
        values=vm((2, patch_rows + 16, tokens), bf16),
        keys=vm((2, tokens, head), bf16),
        queries=vm((2, head, tokens), bf16),
        scores=vm((2, held_rows, 2 * frame), f32),
        powers=vm((2, held_rows, 2 * frame), bf16),
        terms=vm((2, n, patch_rows, frame), bf16),
        term_parts=vm((2, n, patch_rows, frame), bf16),
        gap=vm((8, 128), f32),
        gaps=vm((n, 8, 128), f32),
        rounded=vm((patch_rows, frame), bf16),
        rounded_other=vm((patch_rows, frame), bf16),
        mixed=vm((nb, quarter, part), bf16),
        quarters=vm((nb, quarter, part), bf16),
        merged=vm((nb, quarter, part), bf16),
    )
    for name, count in dict(
        piece0=1, piece1=1, piece2=1, spread=1, sums0=1, sums1=1, give0=1, give1=1, gap=1,
        held=1, swap=1, plane=nb, across=1, back=nb, chain=chips, share=1,
    ).items():
        scratch["s_" + name] = pltpu.SemaphoreType.DMA((1,))
        scratch["r_" + name] = pltpu.SemaphoreType.DMA((count,))
    names = ("timesteps", *LOADS, *outputs, *scratch)
    difference, grad = pl.pallas_call(
        functools.partial(main_kernel, n, nb, part, names),
        out_shape=list(outputs.values()),
        in_specs=[pl.BlockSpec(memory_space=pltpu.SMEM)]
        + [pl.BlockSpec(memory_space=pltpu.HBM)] * len(LOADS),
        out_specs=[pl.BlockSpec(memory_space=pltpu.VMEM)] * 2,
        scratch_shapes=list(scratch.values()),
        compiler_params=pltpu.CompilerParams(
            collective_id=0, has_side_effects=True, vmem_limit_bytes=60 * 1024 * 1024
        ),
    )(timesteps, *(pltpu.with_memory_space_constraint(inputs[x], pltpu.HBM) for x in LOADS))
    weight_grad, difference = pl.pallas_call(
        functools.partial(last_kernel, part),
        out_shape=[
            jax.ShapeDtypeStruct((patch_rows, width), f32),
            jax.ShapeDtypeStruct((patch_rows, frame), f32),
        ],
        in_specs=[pl.BlockSpec(memory_space=pltpu.VMEM)] * 2,
        out_specs=[pl.BlockSpec(memory_space=pl.ANY)] * 2,
        scratch_shapes=[vm((patch_rows, width), f32), pltpu.SemaphoreType.DMA((chunks + 1,))],
        compiler_params=pltpu.CompilerParams(vmem_limit_bytes=8 * 1024 * 1024),
    )(*(pltpu.with_memory_space_constraint(x, pltpu.VMEM) for x in (grad, difference)))
    return (difference[None], weight_grad)


def solution(mesh):
    in_specs = (
        P("batch", "tm", None),
        P(),
        P("batch", None, "tm"),
        P("batch"),
        P(),
        P("tm", None, None),
        P(None, "tm"),
        P(None, "tm"),
        P(None, "tm"),
        P("tm", None),
        P(None, "tm"),
        P(),
        P(),
        P("tm", None, None),
        P(None, "tm"),
        P(None, "tm"),
        P(None, "tm"),
        P("tm", None),
        P(None, "tm"),
        P(),
    )
    out_specs = (P("batch", None, "tm"), P())
    return jax.shard_map(
        per_device, mesh=mesh, in_specs=in_specs, out_specs=out_specs, check_vma=False
    )
```

```python
import functools
import math

import jax
import jax.numpy as jnp
from jax import lax
from jax.experimental import pallas as pl
from jax.experimental.pallas import tpu as pltpu
from jax.sharding import PartitionSpec as P

HD = 128
FREQ = 256

norm_floor = 0.05
gap_floor = 0.25

MESH = pl.DeviceIdType.MESH
f32 = jnp.float32
bf16 = jnp.bfloat16


def hail(sizes):
    barrier = pltpu.get_barrier_semaphore()
    for axis, size in sizes.items():
        me = lax.axis_index(axis)
        for k in range(1, size):
            pl.semaphore_signal(
                barrier, inc=1, device_id={axis: lax.rem(me + k, size)}, device_id_type=MESH
            )


def meet(sizes):
    count = sum(size - 1 for size in sizes.values())
    pl.semaphore_wait(pltpu.get_barrier_semaphore(), count)


def partner(me, k, size):
    if size & (size - 1):
        return lax.rem(me + k, size)
    peer, bit = me, 1
    while bit < size:
        if k & bit:
            peer = peer + bit - 2 * bit * lax.rem(lax.div(me, bit), 2)
        bit *= 2
    return peer


class Exchange:
    def __init__(self, axis, size, source, slots, sems):
        self.axis, self.size, self.source, self.slots, self.sems = axis, size, source, slots, sems

    def start(self):
        me = lax.axis_index(self.axis)
        for k in range(self.size - 1, 0, -1):
            peer = partner(me, k, self.size)
            self.copy(self.source(peer), self.slots.at[me], peer).start()
        return self

    def copy(self, source, target, peer):
        return pltpu.make_async_remote_copy(
            src_ref=source,
            dst_ref=target,
            send_sem=self.sems[0].at[0],
            recv_sem=self.sems[1].at[0],
            device_id={self.axis: peer},
            device_id_type=MESH,
        )

    def all(self):
        both = self.slots.at[pl.ds(0, self.size - 1)]
        return self.copy(both, both, lax.axis_index(self.axis))


def exchange(axis, size, source, slots, sems):
    return Exchange(axis, size, source, slots, sems).start()


def landed(copies):
    copies.all().wait_recv()


def gone(copies):
    copies.all().wait_send()


def split(wide):
    high = wide.astype(bf16)
    return high, (wide - high.astype(f32)).astype(bf16)


def dot_nt(left, right):
    return lax.dot_general(left, right, (((1,), (1,)), ((), ())), preferred_element_type=f32)


def dot(left, right):
    return jnp.dot(left, right, preferred_element_type=f32)


LOADS = (
    "time0", "time1", "hidden", "gen", "noise", "embed0", "proj0", "embed1",
    "proj1", "query0", "key0", "query1", "key1", "value0", "out0", "value1", "out1", "gain0", "gain1",
)


def main_kernel(n, nb, part, names, *refs):
    r = dict(zip(names, refs, strict=True))
    me = lax.axis_index("tm")
    mine = lax.axis_index("batch")
    core, chip = lax.rem(me, 2), lax.div(me, 2)
    chips = n // 2
    hidden, stack = r["v_hidden"], r["stack"]
    noisy_ref = r["noisy"]
    patch_rows, frame = noisy_ref.shape
    tokens = n * frame
    kin = 2 * patch_rows
    width = hidden.shape[1]
    chunks = width // part
    head = r["v_query0"].shape[1]
    freq_rows = r["v_time0"].shape[1]
    loads = {}
    for i, name in enumerate(LOADS):
        loads[name] = pltpu.make_async_copy(r[name], r["v_" + name], r["load_sem"].at[i])
        loads[name].start()
    hail({"tm": n, "batch": nb})

    def sem(name):
        return r["s_" + name], r["r_" + name]

    half = FREQ // 2
    time_step = jnp.full((16, half), r["timesteps"][0], jnp.int32).astype(f32)
    place = lax.broadcasted_iota(jnp.int32, (16, half), 1)
    angles = time_step
    bit = 1
    while bit < half:
        factor = math.exp(-math.log(10000.0) * bit / half)
        angles = angles * jnp.where(lax.rem(lax.div(place, bit), 2) == 1, factor, 1.0)
        bit *= 2
    wave = jnp.concatenate([jnp.cos(angles), jnp.sin(angles)], axis=1).astype(bf16)
    raw = time_step[:8] * (1.0 / 1000.0)
    level = ((5.0 * raw) / (1.0 + 4.0 * raw))[:1, :1]
    picked = (2 * half, 3 * freq_rows)
    column = lax.rem(lax.broadcasted_iota(jnp.int32, picked, 1), freq_rows) + me * freq_rows
    chosen = (lax.broadcasted_iota(jnp.int32, picked, 0) == column).astype(f32).astype(bf16)
    own_wave = dot(wave, chosen)
    own_wave = jnp.concatenate([own_wave, own_wave], axis=0)
    block_of = lax.broadcasted_iota(jnp.int32, own_wave.shape, 1) // freq_rows
    row_of = lax.broadcasted_iota(jnp.int32, own_wave.shape, 0)
    share = None
    for i in (0, 1):
        loads[f"time{i}"].wait()
        table = r[f"v_time{i}"]
        early = (row_of // 8 == i) & (lax.rem(row_of, 2) == block_of)
        late = (row_of // 8 == 2) & (lax.rem(row_of, 2) == i) & (block_of == 2)
        left = jnp.where(early | late, own_wave, 0.0).astype(bf16)
        if freq_rows % 16:
            for j in range(3):
                term = dot(left[:, j * freq_rows : (j + 1) * freq_rows], table[j])
                share = term if share is None else share + term
        else:
            term = dot(left, table[...].reshape(3 * freq_rows, width))
            share = term if share is None else share + term
    pieces, piece_parts = r["pieces"], r["piece_parts"]
    some = width // 4
    line = lax.broadcasted_iota(jnp.int32, (8, some), 0) // 2
    for g in range(3):
        rows = share[8 * g : 8 * g + 8]
        picked = rows[:, :some]
        for q in range(1, 4):
            picked = jnp.where(line == q, rows[:, q * some : (q + 1) * some], picked)
        pieces[g] = picked.astype(bf16)
    meet({"tm": n, "batch": nb})

    def hand_on(g):
        copies = exchange("tm", n, lambda peer: pieces.at[g], piece_parts.at[g], sem(f"piece{g}"))
        piece_parts[g, me] = pieces[g]
        return copies

    piece_copies = [hand_on(0)]

    loads["hidden"].wait()
    loads["gen"].wait()
    loads["noise"].wait()
    made = dot_nt(hidden[...], r["v_gen"][...]).T.astype(bf16).astype(f32)
    noisy = ((1.0 - level) * made + level * r["v_noise"][...].astype(f32)).astype(bf16)
    noisy_ref[...] = noisy
    patches = r["patches"]
    spread = exchange("tm", n, lambda peer: noisy_ref, patches, sem("spread"))
    patches[me] = noisy_ref[...]
    piece_copies.extend([hand_on(1), hand_on(2)])
    noisy = noisy.astype(f32)

    def columns(s):
        return pl.ds(pl.multiple_of(s * part, 128), part)

    held = r["held"]
    other = {"tm": me + 1 - 2 * core}

    def send(name, source, target, at, where, slot=0):
        return pltpu.make_async_remote_copy(
            src_ref=source,
            dst_ref=target,
            send_sem=r["s_" + name].at[slot],
            recv_sem=r["r_" + name].at[at],
            device_id=where,
            device_id_type=MESH,
        )

    def part_of(q, side):
        return columns(lax.rem(2 * q + side, chunks))

    gram = r["gram"]
    extra = kin + patch_rows

    def gram_of(i):
        embed, proj = r[f"v_embed{i}"], r[f"v_proj{i}"]
        loads[f"embed{i}"].wait()
        loads[f"proj{i}"].wait()
        ones = jnp.ones((16, width), bf16)
        gram[i] = dot_nt(jnp.concatenate([embed[...], proj[...], ones], axis=0), embed[...])

    gram_of(0)
    for q in range(chips):
        send("held", hidden.at[:, part_of(q, 1 - core)], held.at[q], 0, other).start()
    gram_of(1)

    block = 2 * frame
    blocks = [slice(s * block, (s + 1) * block) for s in range(tokens // block)]
    rscale = r["rscale"]
    means, centered = [], []
    for i in (0, 1):
        mean_row = gram[i, extra : extra + 8] / width
        means.append(mean_row.T[:, :1])
        centered.append(gram[i, :kin] / width - means[i] * mean_row[:1])

    left_ref, fold, fold_v, gate_fold = r["left"], r["fold"], r["fold_v"], r["gate_fold"]
    qk, squares, square_parts = r["qk"], r["squares"], r["square_parts"]

    def fold_qk(i):
        embed, query, key = r[f"v_embed{i}"], r[f"v_query{i}"], r[f"v_key{i}"]
        landed(piece_copies[i])
        modul = jnp.sum(piece_parts[i].astype(f32), axis=0)
        line = lax.broadcasted_iota(jnp.int32, (16, some), 0)
        for q in range(4):
            at = slice(q * some, (q + 1) * some)
            shift, scale = modul[2 * q : 2 * q + 1], modul[2 * q + 1 : 2 * q + 2]
            left_ref[i, :kin, at] = (
                (embed[:, at].astype(f32) - means[i]) * (1.0 + scale)
            ).astype(bf16)
            shift_high, shift_low = split(shift)
            left_ref[i, kin:, at] = jnp.where(
                line == 0, shift_high.astype(f32), jnp.where(line == 1, shift_low.astype(f32), 0.0)
            ).astype(bf16)
        fold[i] = dot(left_ref[i], jnp.concatenate([query[...], key[...]], axis=1))

    def project_qk(i):
        folded = jnp.concatenate(split(fold[i, :kin].T), axis=1)
        tail = fold[i, kin : kin + 8].T
        offset = tail[:, :1] + tail[:, 1:2]
        for at in blocks:
            full = dot(folded, stack[:, at]) * rscale[i : i + 1, at] + offset
            qk[i, :, at] = full
            found = [full[j * head : (j + 1) * head] for j in range(2)]
            found = [jnp.sum(rows * rows, axis=0, keepdims=True) for rows in found]
            squares[i, :, at] = jnp.concatenate(found, axis=0).astype(squares.dtype)
        copies = exchange(
            "tm", n, lambda peer: squares.at[i], square_parts.at[i], sem(f"sums{i}")
        )
        square_parts[i, me] = squares[i]
        return copies

    values = r["values"]

    def fold_value(i):
        fold_v[i] = dot(left_ref[i], r[f"v_value{i}"][...])

    def fold_gate(i):
        out, proj = r[f"v_out{i}"], r[f"v_proj{i}"]
        gated = []
        for q in range(4):
            at = slice(q * some, (q + 1) * some)
            gate = gate_sum[2 * q + i : 2 * q + i + 1]
            gated.append((proj[:, at].astype(f32) * gate).astype(bf16))
        gate_fold[i] = dot_nt(out[...], jnp.concatenate(gated, axis=1))

    def join(i):
        gate_high, gate_low = split(gate_fold[i].T)
        value_high, value_low = split(fold_v[i])
        both = dot_nt(jnp.concatenate([gate_high, gate_low], axis=0), value_high)
        joint = both[:patch_rows] + both[patch_rows:] + dot_nt(gate_high, value_low)
        offset = joint[:, kin : kin + 1] + joint[:, kin + 1 : kin + 2]
        pairs = jnp.concatenate(split(joint[:, :kin]), axis=1)
        for at in blocks:
            full = dot(pairs, stack[:, at]) * rscale[i : i + 1, at] + offset
            values[i, :patch_rows, at] = full.astype(bf16)
            values[i, patch_rows:, at] = jnp.ones((16, block), bf16)

    loads["query0"].wait()
    loads["key0"].wait()
    fold_qk(0)
    for name in LOADS[LOADS.index("query1") :]:
        loads[name].wait()
    landed(spread)
    for s in range(n):
        at = slice(s * frame, (s + 1) * frame)
        now = patches[s]
        before = patches[s - 1] if s else jnp.zeros_like(now)
        both = jnp.concatenate([now, before], axis=0)
        stack[:kin, at] = both
        stack[kin:, at] = both
    for i in (0, 1):
        gram_pair = jnp.concatenate(split(centered[i]), axis=1)
        for at in blocks:
            pair = stack[:, at]
            variance = jnp.sum(pair[:kin].astype(f32) * dot(gram_pair, pair), axis=0, keepdims=True)
            rscale[i : i + 1, at] = lax.rsqrt(jnp.maximum(variance, 0.0) + norm_floor)
    sums = [project_qk(0)]
    fold_value(0)
    fold_qk(1)
    sums.append(project_qk(1))

    groups = min(4, tokens // block)
    per_group = tokens // block // groups
    keys, terms, term_parts = r["keys"], r["terms"], r["term_parts"]

    starts = [block * b * (b + 1) // 2 for b in range(tokens // block)]

    def prepare(i):
        inverse = lax.rsqrt(
            jnp.sum(square_parts[i].astype(f32), axis=0) / (head * n) + norm_floor
        )
        gain = r[f"v_gain{i}"]
        gains = gain[0:1, :] * gain[1:2, :]
        to_query = math.log2(math.e) / math.sqrt(HD)
        for at in blocks:
            gained = qk[i, head:, at] * inverse[1:2, at]
            keys[i, at, :] = (gained.T * gains).astype(bf16)
            r["queries"][i, :, at] = (qk[i, :head, at] * (inverse[:1, at] * to_query)).astype(bf16)

    def put(i, b, powers, length):
        summed = dot(values[i, :, :length], powers)
        term = (summed[:patch_rows] / summed[patch_rows : patch_rows + 1]).astype(bf16)
        for j in range(2):
            terms[i, 2 * b + j] = term[:, j * frame : (j + 1) * frame]

    def score(i):
        early = lax.broadcasted_iota(jnp.int32, (frame, block), 1) < frame
        for b, (at, start) in enumerate(zip(blocks, starts)):
            length = (b + 1) * block
            scores = dot(keys[i, :length], r["queries"][i, :, at])
            r["scores"][i, start : start + length - frame] = scores[: length - frame]
            edge = jnp.where(early, -1e30, scores[length - frame :])
            r["scores"][i, start + length - frame : start + length] = edge

    def soften(i):
        for b, start in enumerate(starts):
            rows = slice(start, start + (b + 1) * block)
            peak = jnp.max(r["scores"][i, rows], axis=0, keepdims=True)
            r["powers"][i, rows] = jnp.exp2(r["scores"][i, rows] - peak).astype(bf16)

    def combine(i):
        for b, start in enumerate(starts):
            length = (b + 1) * block
            put(i, b, r["powers"][i, start : start + length], length)

    def looped(i):
        for group in range(groups):
            length = (group + 1) * per_group * block
            low = length - per_group * block

            def block_step(b, carry):
                at = pl.ds(pl.multiple_of(b * block, block), block)
                scores = dot(keys[i, :length], r["queries"][i, :, at])
                shape = (length - low, block)
                key_frame = (lax.broadcasted_iota(jnp.int32, shape, 0) + low) // frame
                query_frame = (lax.broadcasted_iota(jnp.int32, shape, 1) + b * block) // frame
                edge = jnp.where(key_frame <= query_frame, scores[low:], -1e30)
                scores = jnp.concatenate([scores[:low], edge], axis=0) if low else edge
                peak = jnp.max(scores, axis=0, keepdims=True)
                put(i, b, jnp.exp2(scores - peak).astype(bf16), length)
                return carry

            lax.fori_loop(group * per_group, (group + 1) * per_group, block_step, 0)

    def hand_out(i):
        copies = exchange(
            "tm", n, lambda peer: terms.at[i, peer], term_parts.at[i], sem(f"give{i}")
        )
        term_parts[i, me] = terms[i, me]
        return copies

    fold_value(1)
    landed(piece_copies[2])
    gate_sum = jnp.sum(piece_parts[2].astype(f32), axis=0)
    landed(sums[0])
    fold_gate(0)
    fold_gate(1)
    prepare(0)
    if per_group == 1:
        score(0)
    join(0)
    join(1)
    give = []
    for i in (0, 1):
        if i:
            landed(sums[i])
            prepare(i)
        if per_group == 1:
            if i:
                score(i)
            soften(i)
            combine(i)
        else:
            looped(i)
        give.append(hand_out(i))

    own = stack[:, pl.ds(pl.multiple_of(me * frame, frame), frame)]
    velocity = []
    for i in (0, 1):
        inner = jnp.concatenate(split(gram[i, kin:extra]), axis=1)
        velocity.append(dot(inner, own))
    for i in (0, 1):
        landed(give[i])
        velocity[i] = velocity[i] + jnp.sum(term_parts[i].astype(f32), axis=0)
    pred_real = noisy - level * velocity[0]
    pred_fake = noisy - level * velocity[1]
    difference = pred_fake - pred_real
    rounded, rounded_other, gap, gaps = r["rounded"], r["rounded_other"], r["gap"], r["gaps"]
    rounded[...] = difference.astype(bf16)
    swap = send("swap", rounded, rounded_other, 0, other)
    swap.start()
    distance = jnp.abs(made - pred_real)
    distance = jnp.sum(jnp.sum(distance, axis=0, keepdims=True), axis=1, keepdims=True)
    gap[...] = jnp.broadcast_to(distance, gap.shape)
    gap_copies = exchange("tm", n, lambda peer: gap, gaps, sem("gap"))
    gaps[me] = gap[...]
    products, partial, gathered = r["products"], r["partial"], r["gathered"]
    hops = [*range(chips - 1, 0, -1), 0]
    for hop in hops:
        products[hop] = dot(rounded[...], hidden[:, part_of(partner(chip, hop, chips), core)])
    all_held = send("held", held, held, 0, other)
    all_held.wait_recv()
    swap.wait_recv()
    order = [*range(nb - 1, 0, -1), 0]
    for hop in hops:
        at = partner(chip, hop, chips)
        whole = products[hop] + dot(rounded_other[...], held[at])
        partial[hop] = whole.reshape(partial.shape[1:]).astype(bf16)
    for k in order:
        piece = partner(mine, k, nb)
        for hop in hops[:-1]:
            where = {"tm": 2 * partner(chip, hop, chips) + core}
            send("plane", partial.at[hop, piece], gathered.at[k, hop], k, where).start()
    landed(gap_copies)
    normalizer = jnp.maximum(jnp.sum(gaps[...], axis=0) / (patch_rows * tokens), gap_floor)
    r["difference"][...] = difference / normalizer[:1, :1]
    factor = 1.0 / (normalizer[:1, :1] * math.sqrt(nb * tokens))
    mixed, quarters, merged, grad = r["mixed"], r["quarters"], r["merged"], r["grad"]
    for k in order:
        piece = partner(mine, k, nb)
        near = gathered.at[k, pl.ds(1, chips - 1)]
        send("plane", near, near, k, other).wait_recv()
        summed = partial[0, piece].astype(f32)
        for hop in hops[:-1]:
            summed = summed + gathered[k, hop].astype(f32)
        summed = (summed * factor).astype(bf16)
        if k:
            mixed[k] = summed
            send("across", mixed.at[k], quarters.at[k], 0, {"batch": piece}).start()
        else:
            quarters[0] = summed
    far = quarters.at[pl.ds(1, nb - 1)]
    across = send("across", far, far, 0, other)
    across.wait_recv()
    merged[mine] = jnp.sum(quarters[...].astype(f32), axis=0).astype(bf16)
    grad[core, chip, mine] = merged[mine]
    back = []
    for k in range(1, nb):
        back.append(
            send("back", merged.at[mine], merged.at[mine], k, {"batch": partner(mine, k, nb)})
        )

    for copy in back[::-1]:
        copy.start()

    def to_chips(piece, k):
        for hop in range(chips - 1, 0, -1):
            where = {"tm": 2 * partner(chip, hop, chips) + core}
            target = grad.at[core, chip, piece]
            send("chain", merged.at[piece], target, k * chips + hop, where).start()
        send("share", merged.at[piece], grad.at[core, chip, piece], 0, other).start()

    to_chips(mine, 0)
    for k in range(1, nb):
        back[k - 1].wait_recv()
        piece = partner(mine, k, nb)
        grad[core, chip, piece] = merged[piece]
        to_chips(piece, k)
    for k in range(nb):
        for hop in range(1, chips):
            slot = grad.at[core, partner(chip, hop, chips), partner(mine, k, nb)]
            send("chain", slot, slot, k * chips + hop, other).wait_recv()
            send("share", slot, slot, 0, other).start()
    whole = send("share", grad.at[core], grad.at[1 - core], 0, other)
    whole.wait_recv()
    for copies in (
        *piece_copies, spread, *sums, *give, gap_copies,
    ):
        gone(copies)
    all_held.wait_send()
    swap.wait_send()
    for k in order:
        near = gathered.at[k, pl.ds(1, chips - 1)]
        send("plane", near, near, k, other).wait_send()
    across.wait_send()
    rest = merged.at[pl.ds(0, nb - 1)]
    send("back", rest, rest, 0, other).wait_send()
    for hop in range(1, chips):
        send("chain", merged, merged, 0, other).wait_send()
    whole.wait_send()


def last_kernel(part, grad_ref, difference_ref, weight_out, difference_out, wide_ref, sems):
    patch_rows, width = wide_ref.shape
    copies = [pltpu.make_async_copy(difference_ref, difference_out, sems.at[0])]
    copies[0].start()
    for s in range(width // part):
        at = slice(s * part, (s + 1) * part)
        wide_ref[:, at] = grad_ref[s % 2, s // 2].reshape(patch_rows, part).astype(f32)
        copies.append(
            pltpu.make_async_copy(wide_ref.at[:, at], weight_out.at[:, at], sems.at[s + 1])
        )
        copies[-1].start()
    for copy in copies:
        copy.wait()


def per_device(
    hidden_states,
    gen_weight,
    noise_field,
    timesteps,
    embed_real,
    time_real,
    query_real,
    key_real,
    value_real,
    out_real,
    gain_real,
    proj_real,
    embed_fake,
    time_fake,
    query_fake,
    key_fake,
    value_fake,
    out_fake,
    gain_fake,
    proj_fake,
):
    n = lax.axis_size("tm")
    nb = lax.axis_size("batch")
    frame = hidden_states.shape[1]
    tokens = frame * n
    patch_rows, width = gen_weight.shape
    part = -(-width // (n * 128)) * 128
    while width % part:
        part += 128
    chunks = width // part
    many = tokens // (2 * frame)
    held_rows = many * (many + 1) * frame if many <= 4 else 16
    chips, quarter, head = n // 2, patch_rows // nb, query_real.shape[1]
    kin = 2 * patch_rows
    inputs = dict(
        time0=time_real.transpose(1, 0, 2), time1=time_fake.transpose(1, 0, 2),
        hidden=hidden_states[0], gen=gen_weight, noise=noise_field[0],
        embed0=embed_real, proj0=proj_real, embed1=embed_fake, proj1=proj_fake,
        query0=query_real, key0=key_real, query1=query_fake, key1=key_fake,
        value0=value_real, out0=out_real, value1=value_fake, out1=out_fake,
        gain0=gain_real, gain1=gain_fake,
    )
    vm = pltpu.VMEM
    outputs = dict(
        difference=vm((patch_rows, frame), f32),
        grad=vm((2, chips, nb, quarter, part), bf16),
    )
    scratch = {}
    for name in LOADS:
        array = inputs[name]
        scratch["v_" + name] = vm(array.shape, array.dtype)
    scratch.update(
        load_sem=pltpu.SemaphoreType.DMA((len(LOADS),)),
        patches=vm((n, patch_rows, frame), bf16),
        pieces=vm((3, 8, width // 4), bf16),
        piece_parts=vm((3, n, 8, width // 4), bf16),
        noisy=vm((patch_rows, frame), bf16),
        held=vm((chips, frame, part), bf16),
        products=vm((chips, patch_rows, part), f32),
        partial=vm((chips, nb, quarter, part), bf16),
        gathered=vm((nb, chips, quarter, part), bf16),
        gram=vm((2, kin + patch_rows + 16, kin), f32),
        stack=vm((2 * kin, tokens), bf16),
        rscale=vm((2, tokens), f32),
        left=vm((2, kin + 16, width), bf16),
        fold=vm((2, kin + 16, 2 * head), f32),
        fold_v=vm((2, kin + 16, head), f32),
        gate_fold=vm((2, head, patch_rows), f32),
        qk=vm((2, 2 * head, tokens), f32),
        squares=vm((2, 2, tokens), bf16),
        square_parts=vm((2, n, 2, tokens), bf16),
        values=vm((2, patch_rows + 16, tokens), bf16),
        keys=vm((2, tokens, head), bf16),
        queries=vm((2, head, tokens), bf16),
        scores=vm((2, held_rows, 2 * frame), f32),
        powers=vm((2, held_rows, 2 * frame), bf16),
        terms=vm((2, n, patch_rows, frame), bf16),
        term_parts=vm((2, n, patch_rows, frame), bf16),
        gap=vm((8, 128), f32),
        gaps=vm((n, 8, 128), f32),
        rounded=vm((patch_rows, frame), bf16),
        rounded_other=vm((patch_rows, frame), bf16),
        mixed=vm((nb, quarter, part), bf16),
        quarters=vm((nb, quarter, part), bf16),
        merged=vm((nb, quarter, part), bf16),
    )
    for name, count in dict(
        piece0=1, piece1=1, piece2=1, spread=1, sums0=1, sums1=1, give0=1, give1=1, gap=1,
        held=1, swap=1, plane=nb, across=1, back=nb, chain=nb * chips, share=1,
    ).items():
        scratch["s_" + name] = pltpu.SemaphoreType.DMA((1,))
        scratch["r_" + name] = pltpu.SemaphoreType.DMA((count,))
    names = ("timesteps", *LOADS, *outputs, *scratch)
    difference, grad = pl.pallas_call(
        functools.partial(main_kernel, n, nb, part, names),
        out_shape=list(outputs.values()),
        in_specs=[pl.BlockSpec(memory_space=pltpu.SMEM)]
        + [pl.BlockSpec(memory_space=pltpu.HBM)] * len(LOADS),
        out_specs=[pl.BlockSpec(memory_space=pltpu.VMEM)] * 2,
        scratch_shapes=list(scratch.values()),
        compiler_params=pltpu.CompilerParams(
            collective_id=0, has_side_effects=True, vmem_limit_bytes=60 * 1024 * 1024
        ),
    )(timesteps, *(pltpu.with_memory_space_constraint(inputs[x], pltpu.HBM) for x in LOADS))
    weight_grad, difference = pl.pallas_call(
        functools.partial(last_kernel, part),
        out_shape=[
            jax.ShapeDtypeStruct((patch_rows, width), f32),
            jax.ShapeDtypeStruct((patch_rows, frame), f32),
        ],
        in_specs=[pl.BlockSpec(memory_space=pltpu.VMEM)] * 2,
        out_specs=[pl.BlockSpec(memory_space=pl.ANY)] * 2,
        scratch_shapes=[vm((patch_rows, width), f32), pltpu.SemaphoreType.DMA((chunks + 1,))],
        compiler_params=pltpu.CompilerParams(vmem_limit_bytes=8 * 1024 * 1024),
    )(*(pltpu.with_memory_space_constraint(x, pltpu.VMEM) for x in (grad, difference)))
    return (difference[None], weight_grad)


def solution(mesh):
    in_specs = (
        P("batch", "tm", None),
        P(),
        P("batch", None, "tm"),
        P("batch"),
        P(),
        P("tm", None, None),
        P(None, "tm"),
        P(None, "tm"),
        P(None, "tm"),
        P("tm", None),
        P(None, "tm"),
        P(),
        P(),
        P("tm", None, None),
        P(None, "tm"),
        P(None, "tm"),
        P(None, "tm"),
        P("tm", None),
        P(None, "tm"),
        P(),
    )
    out_specs = (P("batch", None, "tm"), P())
    return jax.shard_map(
        per_device, mesh=mesh, in_specs=in_specs, out_specs=out_specs, check_vma=False
    )
```
